128 devices in a mesh: rep: 2 (over core), rows: 64 (over z, y, x).
Axes of the slice: x: 4, y: 4, z: 4, core: 2. Of those that a mesh axis runs over, the one named last changes fastest.
Arguments:
- adjacency: bfloat16 [24576, 24576], P('rows', 'rep')
- block_mask: int32 [64, 64], replicated
- features: bfloat16 [24576, 200], P('rows')
- w_one: bfloat16 [200, 512], replicated
- w_two: bfloat16 [512, 107], replicated
Outputs:
- output: float32 [24576, 107], P('rows')
All inputs are finite; a program needn't handle non-finite values.
Results may differ from the reference program's by a relative error of at most 0.001.
Values are sent between devices in bfloat16 or wider.
A program may use at most 1 GiB of HBM per device.

```python
import jax
import jax.numpy as jnp
from jax import lax

ROWS = 64
BLOCK = 384
F0 = 200
F1 = 512
F2 = 107

NODES = ROWS * BLOCK


def draw_mask(key):
    key_w, key_r = jax.random.split(key)
    weight = jax.random.randint(key_w, (ROWS,), 1, 5, dtype=jnp.int32)
    pair_draws = jnp.triu(jax.random.randint(key_r, (ROWS, ROWS), 0, 10, dtype=jnp.int32), 1)
    pair_draws = pair_draws + pair_draws.T
    block_ids = jnp.arange(ROWS)
    diag_pair = block_ids[:, None] == block_ids[None, :]
    keep_pair = pair_draws < weight[:, None] + weight[None, :]
    return (keep_pair | diag_pair).astype(jnp.int32)


def hash_rows(row_x, row_y, node_x, node_y):
    hash_bits = row_x[:, None] * node_x[None, :] + (row_y[:, None] ^ node_y[None, :])
    hash_bits = hash_bits ^ (hash_bits >> 15)
    hash_bits = hash_bits * 73244475
    return hash_bits ^ (hash_bits >> 13)


def build_adjacency(key, block_mask):
    key_x, key_y = jax.random.split(key)
    node_x = jax.random.randint(key_x, (NODES,), 0, 2 ** 30, dtype=jnp.int32)
    node_y = jax.random.randint(key_y, (NODES,), 0, 2 ** 30, dtype=jnp.int32)
    col_ids = jnp.arange(NODES)

    def edge_rows(blk_idx):
        row_start = blk_idx * BLOCK
        row_ids = row_start + jnp.arange(BLOCK)
        hash_bits = hash_rows(lax.dynamic_slice_in_dim(node_x, row_start, BLOCK), lax.dynamic_slice_in_dim(node_y, row_start, BLOCK), node_x, node_y)
        col_keep = jnp.repeat(block_mask[blk_idx], BLOCK) == 1
        self_loop = row_ids[:, None] == col_ids[None, :]
        linked = ((hash_bits & 7) == 0) & col_keep[None, :] & jnp.logical_not(self_loop)
        return (linked | self_loop).astype(jnp.float32)

    degree = lax.map(lambda blk_idx: jnp.sum(edge_rows(blk_idx), axis=1), jnp.arange(ROWS)).reshape(NODES)
    inv_root = lax.rsqrt(degree)

    def scaled_rows(blk_idx):
        row_scale = lax.dynamic_slice_in_dim(inv_root, blk_idx * BLOCK, BLOCK)
        return (edge_rows(blk_idx) * row_scale[:, None] * inv_root[None, :]).astype(jnp.bfloat16)

    adjacency = lax.map(scaled_rows, jnp.arange(ROWS)).reshape(NODES, NODES)
    return adjacency, jnp.mean(degree)


def setup_inputs(seed: int = 0) -> dict:
    key_mask, key_adj, key_feat, key_one, key_two = jax.random.split(jax.random.key(seed), 5)
    block_mask = draw_mask(key_mask)
    adjacency, mean_degree = build_adjacency(key_adj, block_mask)
    features = jax.random.normal(key_feat, (NODES, F0), jnp.float32).astype(jnp.bfloat16)
    w_one = (jax.random.normal(key_one, (F0, F1), jnp.float32) * jnp.sqrt(mean_degree / F0)).astype(jnp.bfloat16)
    w_two = (jax.random.normal(key_two, (F1, F2), jnp.float32) * (F1 ** -0.5)).astype(jnp.bfloat16)
    return {'adjacency': adjacency, 'block_mask': block_mask, 'features': features, 'w_one': w_one, 'w_two': w_two}


def reference(adjacency, block_mask, features, w_one, w_two):
    adj_blocks = adjacency.reshape(ROWS, BLOCK, NODES)

    def aggregate(feat_table):
        feat_width = feat_table.shape[1]
        feat_blocks = feat_table.reshape(ROWS, BLOCK, feat_width)

        def one_block(block_pair):
            adj_rows, mask_row = block_pair
            masked = (feat_blocks * mask_row.astype(feat_table.dtype)[:, None, None]).reshape(NODES, feat_width)
            return jnp.dot(adj_rows, masked, preferred_element_type=jnp.float32)

        return lax.map(one_block, (adj_blocks, block_mask)).reshape(NODES, feat_width)

    y_one = aggregate(features).astype(jnp.bfloat16)
    z_one = jnp.maximum(jnp.dot(y_one, w_one, preferred_element_type=jnp.float32), 0.0).astype(jnp.bfloat16)
    y_two = aggregate(z_one).astype(jnp.bfloat16)
    return jnp.dot(y_two, w_two, preferred_element_type=jnp.float32)
```

```python
import jax
import jax.numpy as jnp
from jax import lax
from jax.sharding import PartitionSpec as P


def solution(mesh):
    rep_size = mesh.shape['rep']
    rows_size = mesh.shape['rows']
    stage_count = rows_size // rep_size
    perm_pairs = [(src_rep * rows_size + src_row, (src_row // stage_count) * rows_size + (src_row % stage_count) * rep_size + src_rep) for src_rep in range(rep_size) for src_row in range(rows_size)]

    def range_rows(feat_blk):
        rep_idx = lax.axis_index('rep')
        piece_rows = feat_blk.shape[0] // rep_size
        send_piece = lax.dynamic_slice_in_dim(feat_blk, rep_idx * piece_rows, piece_rows, 0)
        recv_piece = lax.ppermute(send_piece, ('rep', 'rows'), perm_pairs)
        return lax.all_gather(recv_piece, 'rows', axis=0, tiled=True)

    def aggregate(adj_local, block_mask, gathered):
        rows_idx = lax.axis_index('rows')
        rep_idx = lax.axis_index('rep')
        blk_rows = adj_local.shape[0]
        feat_width = gathered.shape[1]
        mask_part = lax.dynamic_slice(block_mask, (rows_idx, rep_idx * stage_count), (1, stage_count))
        masked = (gathered.reshape(stage_count, blk_rows, feat_width) * mask_part.astype(gathered.dtype).reshape(stage_count, 1, 1)).reshape(stage_count * blk_rows, feat_width)
        part_sum = jnp.dot(adj_local, masked, preferred_element_type=jnp.float32)
        return lax.psum(part_sum, 'rep').astype(jnp.bfloat16)

    def local_fn(adj_local, block_mask, feat_blk, w_one, w_two):
        y_one = range_rows(aggregate(adj_local, block_mask, range_rows(feat_blk)))
        z_one = jnp.maximum(jnp.dot(y_one, w_one, preferred_element_type=jnp.float32), 0.0).astype(jnp.bfloat16)
        y_two = aggregate(adj_local, block_mask, z_one)
        return jnp.dot(y_two, w_two, preferred_element_type=jnp.float32)

    return jax.shard_map(local_fn, mesh=mesh, in_specs=(P('rows', 'rep'), P(), P('rows', None), P(), P()), out_specs=P('rows', None), check_vma=False)
```

```python
import jax
import jax.numpy as jnp
from jax import lax
from jax.experimental import pallas as pl
from jax.experimental.pallas import tpu as pltpu
from jax.sharding import PartitionSpec as P

BLOCK = 384
F0, F1, F2 = 200, 512, 107
PART = 128
SLOTS = 96
CHUNK = 4
AXES = ('xyz', 'yzx', 'zxy')
MESH = pl.DeviceIdType.MESH

SRC_ORDER = [
    (0, 0, 0, 0), (1, 0, 0, 0), (2, 0, 0, 0), (0, 0, 0, 1), (0, 0, 0, 3), (0, 0, 1, 0), (0, 0, 3, 0), (0, 1, 0, 0), (1, 0, 0, 1), (1, 0, 0, 3), (1, 0, 1, 0), (1, 0, 3, 0),
    (1, 1, 0, 0), (2, 0, 0, 1), (2, 0, 0, 3), (2, 0, 1, 0), (2, 0, 3, 0), (2, 1, 0, 0), (0, 0, 1, 1), (0, 0, 3, 1), (0, 1, 0, 1), (0, 0, 0, 2), (0, 0, 1, 3), (0, 0, 3, 3),
    (0, 1, 0, 3), (1, 0, 1, 1), (1, 0, 0, 2), (0, 0, 2, 0), (0, 1, 1, 0), (1, 0, 3, 1), (2, 0, 1, 1), (1, 0, 1, 3), (0, 1, 3, 0), (1, 0, 2, 0), (2, 0, 1, 3), (1, 0, 3, 3),
    (1, 1, 0, 1), (1, 1, 1, 0), (2, 0, 3, 1), (1, 1, 3, 0), (2, 1, 1, 0), (1, 1, 0, 3), (2, 0, 3, 3), (0, 0, 2, 1), (2, 1, 0, 1), (0, 1, 1, 1), (2, 0, 0, 2), (0, 0, 1, 2),
    (1, 0, 1, 2), (2, 0, 2, 0), (0, 1, 3, 1), (0, 0, 2, 3), (1, 0, 3, 2), (2, 1, 3, 0), (2, 1, 0, 3), (0, 0, 3, 2), (0, 1, 0, 2), (1, 0, 2, 1), (2, 0, 2, 1), (1, 0, 2, 3),
    (1, 1, 0, 2), (2, 0, 2, 3), (0, 1, 1, 3), (1, 1, 1, 3), (1, 1, 1, 1), (2, 1, 2, 0), (0, 1, 3, 3), (1, 1, 3, 1), (2, 1, 3, 1), (1, 1, 3, 3), (0, 1, 2, 0), (2, 0, 3, 2),
    (2, 1, 1, 1), (2, 0, 1, 2), (2, 1, 0, 2), (1, 1, 2, 0), (2, 1, 3, 3), (0, 0, 2, 2), (2, 1, 1, 3), (2, 1, 2, 1), (1, 0, 2, 2), (0, 1, 2, 1), (2, 0, 2, 2), (1, 1, 1, 2),
    (1, 1, 2, 1), (0, 1, 1, 2), (2, 1, 2, 3), (1, 1, 3, 2), (0, 1, 2, 3), (1, 1, 2, 3), (0, 1, 3, 2), (2, 1, 1, 2), (2, 1, 3, 2), (0, 1, 2, 2), (1, 1, 2, 2), (2, 1, 2, 2),
]
SINK_ORDER = [
    (0, 0, 0, 0), (1, 0, 0, 0), (2, 0, 0, 0), (0, 0, 0, 1), (0, 0, 0, 3), (0, 0, 1, 0), (1, 0, 0, 1), (1, 0, 0, 3), (0, 0, 3, 0), (2, 0, 1, 0), (0, 1, 0, 0), (1, 0, 1, 0),
    (2, 0, 0, 1), (2, 0, 3, 0), (1, 0, 3, 0), (2, 0, 0, 3), (0, 1, 0, 1), (1, 1, 0, 0), (2, 1, 0, 0), (0, 0, 1, 1), (0, 0, 3, 1), (2, 0, 3, 1), (1, 0, 0, 2), (0, 0, 0, 2),
    (0, 1, 0, 3), (2, 0, 2, 0), (0, 0, 1, 3), (2, 0, 1, 1), (1, 0, 1, 1), (1, 0, 1, 3), (0, 0, 3, 3), (2, 0, 3, 3), (0, 1, 1, 0), (0, 0, 2, 0), (1, 0, 3, 1), (2, 0, 1, 3),
    (1, 0, 3, 3), (1, 0, 2, 0), (2, 1, 3, 0), (2, 0, 0, 2), (0, 1, 3, 0), (0, 0, 2, 1), (1, 1, 0, 1), (2, 1, 1, 0), (1, 1, 0, 3), (0, 1, 1, 1), (1, 1, 1, 0), (2, 1, 0, 1),
    (2, 1, 0, 3), (0, 0, 1, 2), (1, 0, 1, 2), (1, 1, 3, 0), (2, 0, 2, 1), (0, 1, 3, 1), (2, 0, 2, 3), (1, 0, 3, 2), (0, 0, 2, 3), (2, 1, 2, 0), (0, 0, 3, 2), (2, 0, 1, 2),
    (2, 0, 3, 2), (1, 0, 2, 1), (0, 1, 0, 2), (1, 1, 0, 2), (1, 0, 2, 3), (0, 1, 1, 3), (2, 1, 1, 1), (2, 1, 3, 1), (2, 1, 0, 2), (0, 1, 1, 2), (0, 1, 3, 3), (0, 1, 2, 0),
    (1, 1, 1, 1), (1, 1, 1, 3), (1, 1, 2, 0), (0, 1, 2, 1), (2, 1, 1, 3), (2, 1, 3, 3), (1, 1, 3, 1), (1, 1, 3, 3), (0, 0, 2, 2), (0, 1, 2, 3), (2, 0, 2, 2), (1, 0, 2, 2),
    (0, 1, 2, 2), (0, 1, 3, 2), (1, 1, 1, 2), (2, 1, 2, 3), (1, 1, 3, 2), (1, 1, 2, 1), (2, 1, 1, 2), (2, 1, 2, 1), (1, 1, 2, 3), (2, 1, 3, 2), (1, 1, 2, 2), (2, 1, 2, 2),
]


def relay_bit(p, axis, off):
    before = AXES[p][:AXES[p].index(axis)]
    return sum(off[a] for a in before) % 2


def piece_sends(is_src, p, zc, dy, dx):
    off = {'x': dx, 'y': dy, 'z': zc}
    order = AXES[p]
    last = -1
    for i, a in enumerate(order):
        if (off[a] != 0) if a != 'z' else (not is_src or zc == 1):
            last = i
    out = []
    if last >= 0:
        a = order[last]
        bit = relay_bit(p, a, off)
        if a in 'xy':
            if off[a] == 3 and bit == 0:
                out.append((a, 1))
            if off[a] == 1 and bit == 1:
                out.append((a, -1))
        elif is_src and zc == 1 and bit == 0:
            out.append(('z', -1))
        elif not is_src and zc == 0 and bit == 1:
            out.append(('z', -1))
    for a in order[last + 1:]:
        out += [(a, 1), (a, -1)]
    return out


def kernel(adj, mask, h0, w1, w2, out, a_v, h0_v, w1_v, w1t, w2_v, tab1, tab2, acc1, acc2, peer1, peer2,
           load_sem, recv_sem1, recv_sem2, send_sem, peer_send, peer_recv):
    rep = lax.axis_index('rep')
    row = lax.axis_index('rows')
    z, y, x = lax.div(row, 16), lax.rem(lax.div(row, 4), 4), lax.rem(row, 4)
    zr = lax.rem(z + 4 - 2 * rep, 4)
    is_src = zr < 2
    near = lax.div(lax.rem(zr + 1, 4), 2)
    inward = 1 - 2 * near
    xs = [lax.rem(x + d, 4) for d in range(4)]
    ys = [lax.rem(y + d, 4) for d in range(4)]
    planes = [near * 48, 48 - near * 48]
    grid = [[[planes[zc] + ys[dy] * 12 + xs[dx] * 3 for dx in range(4)] for dy in range(4)] for zc in range(2)]

    def rows_at(axis, d):
        if axis == 'x':
            return z * 16 + y * 4 + xs[d % 4]
        if axis == 'y':
            return z * 16 + ys[d % 4] * 4 + x
        return lax.rem(z + d * inward + 4, 4) * 16 + y * 4 + x

    links = [('x', 1), ('x', -1), ('y', 1), ('y', -1), ('z', 1), ('z', -1)]
    target = {link: rows_at(*link) for link in links}

    barrier = pltpu.get_barrier_semaphore()
    for link in links:
        pl.semaphore_signal(barrier, inc=1, device_id=(rep, target[link]), device_id_type=MESH)
    pl.semaphore_signal(barrier, inc=1, device_id=(1 - rep, row), device_id_type=MESH)

    loads = [(h0, h0_v), (w1, w1_v), (w2, w2_v), (adj, a_v)]
    loads = [pltpu.make_async_copy(src, dst, load_sem.at[i]) for i, (src, dst) in enumerate(loads)]
    for copy in loads:
        copy.start()

    def slot_of(word):
        p, zc, dy, dx = word
        return grid[zc][dy][dx] + p

    def send_piece(layer, tab, recv_sem, src_role, word):
        slot = slot_of(word)
        for link in piece_sends(src_role, *word):
            pltpu.make_async_remote_copy(
                src_ref=tab.at[slot], dst_ref=tab.at[slot],
                send_sem=send_sem.at[layer, 'xyz'.index(link[0])], recv_sem=recv_sem.at[slot],
                device_id=(rep, target[link]), device_id_type=MESH).start()

    def wait_piece(tab, recv_sem, word):
        slot = slot_of(word)
        pltpu.make_async_copy(tab.at[slot], tab.at[slot], recv_sem.at[slot]).wait()

    own = [(p, 0, 0, 0) for p in range(3)]

    loads[0].wait()

    @pl.when(is_src)
    def _():
        for p in range(3):
            part = h0_v[p * PART:(p + 1) * PART, :].astype(jnp.float32)
            tab1[slot_of(own[p])] = part.T.astype(jnp.bfloat16)

    pl.semaphore_wait(barrier, 7)

    @pl.when(is_src)
    def _():
        for p in range(3):
            send_piece(0, tab1, recv_sem1, True, own[p])

    loads[1].wait()
    w1t[...] = w1_v[...].astype(jnp.float32).T.astype(jnp.bfloat16)
    acc1[...] = jnp.zeros_like(acc1)
    acc2[...] = jnp.zeros_like(acc2)

    def chunk_operands(tab, first):
        a_parts, t_parts = [], []
        for n in range(first, first + CHUNK):
            slot = lax.select(is_src, slot_of(SRC_ORDER[n]), slot_of(SINK_ORDER[n]))
            keep = mask[row, rep * 32 + lax.div(slot, 3)].astype(jnp.float32).astype(jnp.bfloat16)
            a_parts.append(a_v[:, pl.ds(pl.multiple_of(slot * PART, PART), PART)])
            t_parts.append(tab[slot] * keep)
        return jnp.concatenate(a_parts, axis=1), jnp.concatenate(t_parts, axis=1)

    def gather(layer, tab, recv_sem, multiply):
        for first in range(0, SLOTS, CHUNK):
            @pl.when(is_src)
            def _():
                for n in range(first, first + CHUNK):
                    if SRC_ORDER[n] not in own:
                        wait_piece(tab, recv_sem, SRC_ORDER[n])
                        send_piece(layer, tab, recv_sem, True, SRC_ORDER[n])

            @pl.when(jnp.logical_not(is_src))
            def _():
                for n in range(first, first + CHUNK):
                    wait_piece(tab, recv_sem, SINK_ORDER[n])
                    send_piece(layer, tab, recv_sem, False, SINK_ORDER[n])

            if layer == 0 and first == 0:
                loads[3].wait()
            multiply(*chunk_operands(tab, first))

    def multiply1(a, t):
        acc1[...] += lax.dot_general(a, t, (((1,), (1,)), ((), ())), preferred_element_type=jnp.float32)

    def multiply2(a, t):
        zt = jnp.dot(w1t[...], t, preferred_element_type=jnp.float32)
        zt = jnp.maximum(zt, 0.0).astype(jnp.bfloat16)
        acc2[...] += lax.dot_general(a, zt, (((1,), (1,)), ((), ())), preferred_element_type=jnp.float32)

    def to_peer(layer, src, dst):
        return pltpu.make_async_remote_copy(
            src_ref=src, dst_ref=dst, send_sem=peer_send.at[layer], recv_sem=peer_recv.at[layer],
            device_id=(1 - rep, row), device_id_type=MESH)

    gather(0, tab1, recv_sem1, multiply1)
    swap1 = to_peer(0, acc1, peer1)

    @pl.when(jnp.logical_not(is_src))
    def _():
        swap1.start()

    @pl.when(is_src)
    def _():
        swap1.wait_recv()
        for p in range(3):
            rows = slice(p * PART, (p + 1) * PART)
            part = acc1[rows, :] + peer1[rows, :]
            tab2[slot_of(own[p])] = part.T.astype(jnp.bfloat16)
        for p in range(3):
            send_piece(1, tab2, recv_sem2, True, own[p])

    gather(1, tab2, recv_sem2, multiply2)
    swap2 = to_peer(1, acc2, peer2)
    swap2.start()
    loads[2].wait()
    swap2.wait_recv()
    y_two = (acc2[...] + peer2[...]).astype(jnp.bfloat16)
    out[...] = jnp.dot(y_two, w2_v[...], preferred_element_type=jnp.float32)

    def drain(role):
        for layer, tab in ((0, tab1), (1, tab2)):
            for i, axis in enumerate('xyz'):
                words = SRC_ORDER if role else SINK_ORDER
                count = sum(link[0] == axis for word in words for link in piece_sends(role, *word))
                ref = tab.at[pl.ds(0, count)]
                pltpu.make_async_copy(ref, ref, send_sem.at[layer, i]).wait()

    @pl.when(is_src)
    def _():
        drain(True)

    @pl.when(jnp.logical_not(is_src))
    def _():
        drain(False)
        swap1.wait_send()

    swap2.wait_send()


def solution(mesh):
    def step(adj, mask, h0, w1, w2):
        any_space = pl.BlockSpec(memory_space=pl.ANY)
        return pl.pallas_call(
            kernel,
            name='gcn',
            out_shape=jax.ShapeDtypeStruct((BLOCK, F2), jnp.float32),
            in_specs=[any_space, pl.BlockSpec(memory_space=pltpu.SMEM), any_space, any_space, any_space],
            out_specs=pl.BlockSpec(memory_space=pltpu.VMEM),
            scratch_shapes=[
                pltpu.VMEM((BLOCK, 32 * BLOCK), jnp.bfloat16),
                pltpu.VMEM((BLOCK, F0), jnp.bfloat16),
                pltpu.VMEM((F0, F1), jnp.bfloat16),
                pltpu.VMEM((F1, F0), jnp.bfloat16),
                pltpu.VMEM((F1, F2), jnp.bfloat16),
                pltpu.VMEM((SLOTS, F0, PART), jnp.bfloat16),
                pltpu.VMEM((SLOTS, F0, PART), jnp.bfloat16),
                pltpu.VMEM((BLOCK, F0), jnp.float32),
                pltpu.VMEM((BLOCK, F1), jnp.float32),
                pltpu.VMEM((BLOCK, F0), jnp.float32),
                pltpu.VMEM((BLOCK, F1), jnp.float32),
                pltpu.SemaphoreType.DMA((4,)),
                pltpu.SemaphoreType.DMA((SLOTS,)),
                pltpu.SemaphoreType.DMA((SLOTS,)),
                pltpu.SemaphoreType.DMA((2, 3)),
                pltpu.SemaphoreType.DMA((2,)),
                pltpu.SemaphoreType.DMA((2,)),
            ],
            compiler_params=pltpu.CompilerParams(
                collective_id=0, has_side_effects=True, vmem_limit_bytes=60 * 1024 * 1024),
        )(adj, mask, h0, w1, w2)

    return jax.shard_map(step, mesh=mesh, in_specs=(P('rows', 'rep'), P(), P('rows', None), P(), P()),
                         out_specs=P('rows', None), check_vma=False)
```

```python
import heapq
import itertools

import jax
import jax.numpy as jnp
from jax import lax
from jax.experimental import pallas as pl
from jax.experimental.pallas import tpu as pltpu
from jax.sharding import PartitionSpec as P

BLOCK = 384
F0, F1, F2 = 200, 512, 107
PART = 128
SLOTS = 96
CHUNK = 4
BAND = 32
LEAD = 6
AXES = ('xyz', 'yzx', 'zxy')
MESH = pl.DeviceIdType.MESH
MODEL = 0.55, 1.6, 0.1


def relay_bit(p, axis, off):
    before = AXES[p][:AXES[p].index(axis)]
    return sum(off[a] for a in before) % 2


def piece_sends(is_src, p, zc, dy, dx):
    off = {'x': dx, 'y': dy, 'z': zc}
    order = AXES[p]
    last = -1
    for i, a in enumerate(order):
        if (off[a] != 0) if a != 'z' else (not is_src or zc == 1):
            last = i
    out = []
    if last >= 0:
        a = order[last]
        bit = relay_bit(p, a, off)
        if a in 'xy':
            if off[a] == 3 and bit == 0:
                out.append((a, 1))
            if off[a] == 1 and bit == 1:
                out.append((a, -1))
        elif is_src and zc == 1 and bit == 0:
            out.append(('z', -1))
        elif not is_src and zc == 0 and bit == 1:
            out.append(('z', -1))
    for a in order[last + 1:]:
        out += [(a, 1), (a, -1)]
    return out


def core_roles():
    roles = {}
    for rep, z, y, x in itertools.product(range(2), range(4), range(4), range(4)):
        zr = (z - 2 * rep) % 4
        near = (zr + 1) % 4 // 2
        roles[rep, z, y, x] = zr < 2, near, 1 - 2 * near
    return roles


def arrival_orders():
    roles = core_roles()
    piece_time, hop_time, turn_time = MODEL
    orders = None
    for _ in range(4):
        arrived = {core: {} for core in roles}
        link_free, clock, place = {}, {}, {}
        events, tick = [], itertools.count()

        def word_of(core, piece):
            p, plane, sy, sx = piece
            return p, int(plane != roles[core][1]), (sy - core[2]) % 4, (sx - core[3]) % 4

        def send(core, piece, now):
            rep, z, y, x = core
            is_src, _, inward = roles[core]
            for axis, d in piece_sends(is_src, *word_of(core, piece)):
                step = d * inward if axis == 'z' else d
                to = {'x': (rep, z, y, (x + step) % 4), 'y': (rep, z, (y + step) % 4, x), 'z': (rep, (z + step) % 4, y, x)}[axis]
                link = z, y, x, axis, step
                link_free[link] = max(now, link_free.get(link, 0.0)) + piece_time
                heapq.heappush(events, (link_free[link] + hop_time, next(tick), to, piece))

        def advance(core, now):
            if orders is None:
                return
            is_src, near, _ = roles[core]
            words = orders[is_src]
            while place[core] < SLOTS:
                p, zc, dy, dx = words[place[core]]
                piece = p, near ^ zc, (core[2] + dy) % 4, (core[3] + dx) % 4
                if piece not in arrived[core]:
                    return
                start = max(clock[core], arrived[core][piece])
                if start > now:
                    heapq.heappush(events, (start, next(tick), core, None))
                    return
                place[core] += 1
                clock[core] = start + (turn_time if place[core] % CHUNK == 0 else 0.0)
                send(core, piece, start)

        for core, (is_src, near, _) in roles.items():
            place[core], clock[core] = 0, 0.0
            for p in range(3 if is_src else 0):
                piece = p, near, core[2], core[3]
                arrived[core][piece] = 0.0
                if orders is None:
                    send(core, piece, 0.0)
            advance(core, 0.0)
        while events:
            now, _, core, piece = heapq.heappop(events)
            if piece is not None:
                arrived[core][piece] = now
                if orders is None:
                    send(core, piece, now)
            advance(core, now)
        times = {True: {}, False: {}}
        for core in roles:
            for piece, now in arrived[core].items():
                times[roles[core][0]].setdefault(word_of(core, piece), []).append(now)
        orders = {role: sorted(t, key=lambda w: (sum(t[w]) / len(t[w]), w)) for role, t in times.items()}
    return orders[True], orders[False], max(max(t.values()) for t in arrived.values())


SRC_ORDER, SINK_ORDER, _ = arrival_orders()


def kernel(adj, mask, h0t, w1, w2t, out, a_v, w1_v, w1t, w2t_v, tab1, tab2, acc1, acc2, peer1, peer2,
           load_sem, adj_sem, own_sem, recv_sem1, recv_sem2, send_sem, peer_send, peer_recv):
    rep = lax.axis_index('rep')
    row = lax.axis_index('rows')
    z, y, x = lax.div(row, 16), lax.rem(lax.div(row, 4), 4), lax.rem(row, 4)
    zr = lax.rem(z + 4 - 2 * rep, 4)
    is_src = zr < 2
    near = lax.div(lax.rem(zr + 1, 4), 2)
    inward = 1 - 2 * near
    xs = [lax.rem(x + d, 4) for d in range(4)]
    ys = [lax.rem(y + d, 4) for d in range(4)]
    planes = [near * 48, 48 - near * 48]
    grid = [[[planes[zc] + ys[dy] * 12 + xs[dx] * 3 for dx in range(4)] for dy in range(4)] for zc in range(2)]

    def rows_at(axis, d):
        if axis == 'x':
            return z * 16 + y * 4 + xs[d % 4]
        if axis == 'y':
            return z * 16 + ys[d % 4] * 4 + x
        return lax.rem(z + d * inward + 4, 4) * 16 + y * 4 + x

    links = [('x', 1), ('x', -1), ('y', 1), ('y', -1), ('z', 1), ('z', -1)]
    target = {link: rows_at(*link) for link in links}

    barrier = pltpu.get_barrier_semaphore()
    for link in links:
        pl.semaphore_signal(barrier, inc=1, device_id=(rep, target[link]), device_id_type=MESH)
    pl.semaphore_signal(barrier, inc=1, device_id=(1 - rep, row), device_id_type=MESH)

    loads = [pltpu.make_async_copy(src, dst, load_sem.at[i]) for i, (src, dst) in enumerate([(w1, w1_v), (w2t, w2t_v)])]
    bands = [pl.ds(i * BAND, BAND) for i in range(BLOCK // BAND)]
    adj_loads = [pltpu.make_async_copy(adj.at[rows], a_v.at[rows], adj_sem.at[i]) for i, rows in enumerate(bands)]

    def slot_of(word):
        p, zc, dy, dx = word
        return grid[zc][dy][dx] + p

    def send_piece(layer, tab, recv_sem, src_role, word):
        slot = slot_of(word)
        for link in piece_sends(src_role, *word):
            pltpu.make_async_remote_copy(
                src_ref=tab.at[slot], dst_ref=tab.at[slot],
                send_sem=send_sem.at[layer, 'xyz'.index(link[0])], recv_sem=recv_sem.at[slot],
                device_id=(rep, target[link]), device_id_type=MESH).start()

    def wait_piece(tab, recv_sem, word):
        slot = slot_of(word)
        pltpu.make_async_copy(tab.at[slot], tab.at[slot], recv_sem.at[slot]).wait()

    own = [(p, 0, 0, 0) for p in range(3)]

    own_loads = [pltpu.make_async_copy(h0t.at[:, pl.ds(p * PART, PART)], tab1.at[slot_of(own[p])], own_sem.at[p]) for p in range(3)]

    @pl.when(is_src)
    def _():
        for copy in own_loads:
            copy.start()

    for copy in loads + adj_loads:
        copy.start()

    @pl.when(is_src)
    def _():
        for copy in own_loads:
            copy.wait()

    pl.semaphore_wait(barrier, 7)

    @pl.when(is_src)
    def _():
        for p in range(3):
            send_piece(0, tab1, recv_sem1, True, own[p])

    loads[0].wait()
    w1t[...] = w1_v[...].astype(jnp.float32).T.astype(jnp.bfloat16)
    acc1[...] = jnp.zeros_like(acc1)
    acc2[...] = jnp.zeros_like(acc2)

    def chunk_operands(tab, first):
        a_parts, t_parts = [], []
        for n in range(first, first + CHUNK):
            slot = lax.select(is_src, slot_of(SRC_ORDER[n]), slot_of(SINK_ORDER[n]))
            keep = mask[row, rep * 32 + lax.div(slot, 3)].astype(jnp.float32).astype(jnp.bfloat16)
            a_parts.append(a_v[:, pl.ds(pl.multiple_of(slot * PART, PART), PART)])
            t_parts.append(tab[slot] * keep)
        return jnp.concatenate(a_parts, axis=1), jnp.concatenate(t_parts, axis=1)

    def relay(layer, tab, recv_sem, chunk):
        words = range(chunk * CHUNK, (chunk + 1) * CHUNK)

        @pl.when(is_src)
        def _():
            for n in words:
                if SRC_ORDER[n] not in own:
                    wait_piece(tab, recv_sem, SRC_ORDER[n])
                    send_piece(layer, tab, recv_sem, True, SRC_ORDER[n])

        @pl.when(jnp.logical_not(is_src))
        def _():
            for n in words:
                wait_piece(tab, recv_sem, SINK_ORDER[n])
                send_piece(layer, tab, recv_sem, False, SINK_ORDER[n])

    def gather(layer, tab, recv_sem, multiply, lead):
        done = 0
        for chunk in range(SLOTS // CHUNK):
            relay(layer, tab, recv_sem, chunk)
            if chunk + 1 < lead:
                continue
            if layer == 0 and done == 0:
                for copy in adj_loads:
                    copy.wait()
            for _ in range(2):
                if done <= chunk:
                    multiply(*chunk_operands(tab, done * CHUNK))
                    done += 1

    def multiply1(a, t):
        acc1[...] += lax.dot_general(a, t, (((1,), (1,)), ((), ())), preferred_element_type=jnp.float32)

    def multiply2(a, t):
        zt = jnp.dot(w1t[...], t, preferred_element_type=jnp.float32)
        zt = jnp.maximum(zt, 0.0).astype(jnp.bfloat16)
        acc2[...] += lax.dot_general(a, zt, (((1,), (1,)), ((), ())), preferred_element_type=jnp.float32)

    def to_peer(layer, src, dst):
        return pltpu.make_async_remote_copy(
            src_ref=src, dst_ref=dst, send_sem=peer_send.at[layer], recv_sem=peer_recv.at[layer],
            device_id=(1 - rep, row), device_id_type=MESH)

    gather(0, tab1, recv_sem1, multiply1, LEAD)
    swap1 = to_peer(0, acc1, peer1)

    @pl.when(jnp.logical_not(is_src))
    def _():
        swap1.start()

    @pl.when(is_src)
    def _():
        swap1.wait_recv()
        for p in range(3):
            rows = slice(p * PART, (p + 1) * PART)
            part = acc1[rows, :] + peer1[rows, :]
            tab2[slot_of(own[p])] = part.T.astype(jnp.bfloat16)
        for p in range(3):
            send_piece(1, tab2, recv_sem2, True, own[p])

    gather(1, tab2, recv_sem2, multiply2, 1)
    swap2 = to_peer(1, acc2, peer2)
    swap2.start()
    loads[1].wait()
    swap2.wait_recv()
    y_two = (acc2[...] + peer2[...]).astype(jnp.bfloat16)
    out[...] = lax.dot_general(w2t_v[...], y_two, (((1,), (1,)), ((), ())), preferred_element_type=jnp.float32)

    def drain(role):
        for layer, tab in ((0, tab1), (1, tab2)):
            for i, axis in enumerate('xyz'):
                words = SRC_ORDER if role else SINK_ORDER
                count = sum(link[0] == axis for word in words for link in piece_sends(role, *word))
                ref = tab.at[pl.ds(0, count)]
                pltpu.make_async_copy(ref, ref, send_sem.at[layer, i]).wait()

    @pl.when(is_src)
    def _():
        drain(True)

    @pl.when(jnp.logical_not(is_src))
    def _():
        drain(False)
        swap1.wait_send()

    swap2.wait_send()


def solution(mesh):
    def step(adj, mask, h0, w1, w2):
        h0t, w2t = h0.T, w2.T
        any_space = pl.BlockSpec(memory_space=pl.ANY)
        return pl.pallas_call(
            kernel,
            name='gcn',
            out_shape=jax.ShapeDtypeStruct((F2, BLOCK), jnp.float32),
            in_specs=[any_space, pl.BlockSpec(memory_space=pltpu.SMEM), any_space, any_space, any_space],
            out_specs=pl.BlockSpec(memory_space=pltpu.VMEM),
            scratch_shapes=[
                pltpu.VMEM((BLOCK, 32 * BLOCK), jnp.bfloat16),
                pltpu.VMEM((F0, F1), jnp.bfloat16),
                pltpu.VMEM((F1, F0), jnp.bfloat16),
                pltpu.VMEM((F2, F1), jnp.bfloat16),
                pltpu.VMEM((SLOTS, F0, PART), jnp.bfloat16),
                pltpu.VMEM((SLOTS, F0, PART), jnp.bfloat16),
                pltpu.VMEM((BLOCK, F0), jnp.float32),
                pltpu.VMEM((BLOCK, F1), jnp.float32),
                pltpu.VMEM((BLOCK, F0), jnp.float32),
                pltpu.VMEM((BLOCK, F1), jnp.float32),
                pltpu.SemaphoreType.DMA((2,)),
                pltpu.SemaphoreType.DMA((BLOCK // BAND,)),
                pltpu.SemaphoreType.DMA((3,)),
                pltpu.SemaphoreType.DMA((SLOTS,)),
                pltpu.SemaphoreType.DMA((SLOTS,)),
                pltpu.SemaphoreType.DMA((2, 3)),
                pltpu.SemaphoreType.DMA((2,)),
                pltpu.SemaphoreType.DMA((2,)),
            ],
            compiler_params=pltpu.CompilerParams(
                collective_id=0, has_side_effects=True, vmem_limit_bytes=60 * 1024 * 1024),
        )(adj, mask, h0t, w1, w2t).T

    return jax.shard_map(step, mesh=mesh, in_specs=(P('rows', 'rep'), P(), P('rows', None), P(), P()),
                         out_specs=P('rows', None), check_vma=False)
```

```python
import jax
import jax.numpy as jnp
from jax import lax
from jax.experimental import pallas as pl
from jax.experimental.pallas import tpu as pltpu
from jax.sharding import PartitionSpec as P

BLOCK = 384
F0, F1, F2 = 200, 512, 107
PART = 128
SLOTS = 96
CHUNK = 4
BAND = 32
LEAD = 6
AXES = ('xyz', 'yzx', 'zxy')
MESH = pl.DeviceIdType.MESH


def relay_bit(p, axis, off):
    before = AXES[p][:AXES[p].index(axis)]
    return sum(off[a] for a in before) % 2


def piece_sends(is_src, p, zc, dy, dx):
    off = {'x': dx, 'y': dy, 'z': zc}
    order = AXES[p]
    last = -1
    for i, a in enumerate(order):
        if (off[a] != 0) if a != 'z' else (not is_src or zc == 1):
            last = i
    out = []
    if last >= 0:
        a = order[last]
        bit = relay_bit(p, a, off)
        if a in 'xy':
            if off[a] == 3 and bit == 0:
                out.append((a, 1))
            if off[a] == 1 and bit == 1:
                out.append((a, -1))
        elif is_src and zc == 1 and bit == 0:
            out.append(('z', -1))
        elif not is_src and zc == 0 and bit == 1:
            out.append(('z', -1))
    for a in order[last + 1:]:
        out += [(a, 1), (a, -1)]
    return out


def words(codes):
    return [(c // 32, c // 16 % 2, c // 4 % 4, c % 4) for c in codes]


SRC_CODES = [
    0, 32, 64, 80, 1, 3, 36, 44, 48, 4, 12, 65, 67, 16, 33, 35, 68, 76, 60, 81, 2, 7, 40, 83,
    84, 52, 5, 45, 15, 19, 92, 13, 37, 66, 17, 8, 49, 71, 47, 28, 69, 20, 39, 79, 82, 51, 77, 56,
    14, 6, 11, 9, 72, 34, 18, 61, 23, 53, 87, 31, 85, 41, 21, 88, 63, 95, 46, 29, 10, 93, 38, 55,
    43, 70, 24, 50, 78, 75, 73, 30, 59, 22, 94, 27, 25, 57, 86, 62, 91, 89, 26, 54, 42, 74, 58, 90,
]
SINK_CODES = [
    64, 32, 0, 65, 80, 67, 44, 68, 36, 48, 33, 76, 3, 1, 35, 81, 83, 12, 60, 40, 66, 4, 52, 16,
    84, 45, 69, 2, 37, 7, 71, 82, 92, 47, 56, 49, 15, 77, 79, 5, 39, 51, 13, 72, 19, 8, 17, 34,
    87, 61, 41, 85, 28, 14, 63, 43, 70, 20, 95, 6, 53, 11, 93, 55, 78, 9, 18, 46, 88, 23, 38, 73,
    59, 94, 75, 31, 57, 50, 86, 21, 29, 30, 10, 22, 27, 91, 62, 42, 89, 24, 25, 74, 54, 58, 90, 26,
]
SRC_ORDER, SINK_ORDER = words(SRC_CODES), words(SINK_CODES)


def kernel(adj, mask, h0t, w1, w2t, out, a_v, w1_v, w1t, w2t_v, tab1, tab2, acc1, acc2, peer1, peer2,
           load_sem, adj_sem, own_sem, recv_sem1, recv_sem2, send_sem, peer_send, peer_recv):
    rep = lax.axis_index('rep')
    row = lax.axis_index('rows')
    z, y, x = lax.div(row, 16), lax.rem(lax.div(row, 4), 4), lax.rem(row, 4)
    zr = lax.rem(z + 4 - 2 * rep, 4)
    is_src = zr < 2
    near = lax.div(lax.rem(zr + 1, 4), 2)
    inward = 1 - 2 * near
    xs = [lax.rem(x + d, 4) for d in range(4)]
    ys = [lax.rem(y + d, 4) for d in range(4)]
    planes = [near * 48, 48 - near * 48]
    grid = [[[planes[zc] + ys[dy] * 12 + xs[dx] * 3 for dx in range(4)] for dy in range(4)] for zc in range(2)]

    def rows_at(axis, d):
        if axis == 'x':
            return z * 16 + y * 4 + xs[d % 4]
        if axis == 'y':
            return z * 16 + ys[d % 4] * 4 + x
        return lax.rem(z + d * inward + 4, 4) * 16 + y * 4 + x

    links = [('x', 1), ('x', -1), ('y', 1), ('y', -1), ('z', 1), ('z', -1)]
    target = {link: rows_at(*link) for link in links}

    barrier = pltpu.get_barrier_semaphore()
    for link in links:
        pl.semaphore_signal(barrier, inc=1, device_id=(rep, target[link]), device_id_type=MESH)
    pl.semaphore_signal(barrier, inc=1, device_id=(1 - rep, row), device_id_type=MESH)

    loads = [pltpu.make_async_copy(src, dst, load_sem.at[i]) for i, (src, dst) in enumerate([(w1, w1_v), (w2t, w2t_v)])]
    bands = [pl.ds(i * BAND, BAND) for i in range(BLOCK // BAND)]
    adj_loads = [pltpu.make_async_copy(adj.at[rows], a_v.at[rows], adj_sem.at[i]) for i, rows in enumerate(bands)]

    def slot_of(word):
        p, zc, dy, dx = word
        return grid[zc][dy][dx] + p

    def send_piece(layer, tab, recv_sem, src_role, word):
        slot = slot_of(word)
        for link in piece_sends(src_role, *word):
            pltpu.make_async_remote_copy(
                src_ref=tab.at[slot], dst_ref=tab.at[slot],
                send_sem=send_sem.at[layer, 'xyz'.index(link[0])], recv_sem=recv_sem.at[slot],
                device_id=(rep, target[link]), device_id_type=MESH).start()

    def wait_piece(tab, recv_sem, word):
        slot = slot_of(word)
        pltpu.make_async_copy(tab.at[slot], tab.at[slot], recv_sem.at[slot]).wait()

    own = [(p, 0, 0, 0) for p in range(3)]

    own_loads = [pltpu.make_async_copy(h0t.at[:, pl.ds(p * PART, PART)], tab1.at[slot_of(own[p])], own_sem.at[p]) for p in range(3)]

    @pl.when(is_src)
    def _():
        for copy in own_loads:
            copy.start()

    for copy in loads + adj_loads:
        copy.start()

    @pl.when(is_src)
    def _():
        for copy in own_loads:
            copy.wait()

    pl.semaphore_wait(barrier, 7)

    @pl.when(is_src)
    def _():
        for p in range(3):
            send_piece(0, tab1, recv_sem1, True, own[p])

    loads[0].wait()
    w1t[...] = w1_v[...].astype(jnp.float32).T.astype(jnp.bfloat16)
    acc1[...] = jnp.zeros_like(acc1)
    acc2[...] = jnp.zeros_like(acc2)

    def chunk_operands(tab, first):
        a_parts, t_parts = [], []
        for n in range(first, first + CHUNK):
            slot = lax.select(is_src, slot_of(SRC_ORDER[n]), slot_of(SINK_ORDER[n]))
            keep = mask[row, rep * 32 + lax.div(slot, 3)].astype(jnp.float32).astype(jnp.bfloat16)
            a_parts.append(a_v[:, pl.ds(pl.multiple_of(slot * PART, PART), PART)])
            t_parts.append(tab[slot] * keep)
        return jnp.concatenate(a_parts, axis=1), jnp.concatenate(t_parts, axis=1)

    def relay(layer, tab, recv_sem, chunk):
        words = range(chunk * CHUNK, (chunk + 1) * CHUNK)

        @pl.when(is_src)
        def _():
            for n in words:
                if SRC_ORDER[n] not in own:
                    wait_piece(tab, recv_sem, SRC_ORDER[n])
                    send_piece(layer, tab, recv_sem, True, SRC_ORDER[n])

        @pl.when(jnp.logical_not(is_src))
        def _():
            for n in words:
                wait_piece(tab, recv_sem, SINK_ORDER[n])
                send_piece(layer, tab, recv_sem, False, SINK_ORDER[n])

    def gather(layer, tab, recv_sem, multiply, lead):
        done = 0
        for chunk in range(SLOTS // CHUNK):
            relay(layer, tab, recv_sem, chunk)
            if chunk + 1 < lead:
                continue
            if layer == 0 and done == 0:
                for copy in adj_loads:
                    copy.wait()
            for _ in range(2):
                if done <= chunk:
                    multiply(*chunk_operands(tab, done * CHUNK))
                    done += 1

    def multiply1(a, t):
        acc1[...] += lax.dot_general(a, t, (((1,), (1,)), ((), ())), preferred_element_type=jnp.float32)

    def multiply2(a, t):
        zt = jnp.dot(w1t[...], t, preferred_element_type=jnp.float32)
        zt = jnp.maximum(zt, 0.0).astype(jnp.bfloat16)
        acc2[...] += lax.dot_general(a, zt, (((1,), (1,)), ((), ())), preferred_element_type=jnp.float32)

    def to_peer(layer, src, dst):
        return pltpu.make_async_remote_copy(
            src_ref=src, dst_ref=dst, send_sem=peer_send.at[layer], recv_sem=peer_recv.at[layer],
            device_id=(1 - rep, row), device_id_type=MESH)

    gather(0, tab1, recv_sem1, multiply1, LEAD)
    swap1 = to_peer(0, acc1, peer1)

    @pl.when(jnp.logical_not(is_src))
    def _():
        swap1.start()

    @pl.when(is_src)
    def _():
        swap1.wait_recv()
        for p in range(3):
            rows = slice(p * PART, (p + 1) * PART)
            part = acc1[rows, :] + peer1[rows, :]
            tab2[slot_of(own[p])] = part.T.astype(jnp.bfloat16)
        for p in range(3):
            send_piece(1, tab2, recv_sem2, True, own[p])

    gather(1, tab2, recv_sem2, multiply2, 1)
    swap2 = to_peer(1, acc2, peer2)
    swap2.start()
    loads[1].wait()
    swap2.wait_recv()
    y_two = (acc2[...] + peer2[...]).astype(jnp.bfloat16)
    out[...] = lax.dot_general(w2t_v[...], y_two, (((1,), (1,)), ((), ())), preferred_element_type=jnp.float32)

    def drain(role):
        for layer, tab in ((0, tab1), (1, tab2)):
            for i, axis in enumerate('xyz'):
                words = SRC_ORDER if role else SINK_ORDER
                count = sum(link[0] == axis for word in words for link in piece_sends(role, *word))
                ref = tab.at[pl.ds(0, count)]
                pltpu.make_async_copy(ref, ref, send_sem.at[layer, i]).wait()

    @pl.when(is_src)
    def _():
        drain(True)

    @pl.when(jnp.logical_not(is_src))
    def _():
        drain(False)
        swap1.wait_send()

    swap2.wait_send()


def solution(mesh):
    def step(adj, mask, h0, w1, w2):
        h0t, w2t = h0.T, w2.T
        any_space = pl.BlockSpec(memory_space=pl.ANY)
        return pl.pallas_call(
            kernel,
            name='gcn',
            out_shape=jax.ShapeDtypeStruct((F2, BLOCK), jnp.float32),
            in_specs=[any_space, pl.BlockSpec(memory_space=pltpu.SMEM), any_space, any_space, any_space],
            out_specs=pl.BlockSpec(memory_space=pltpu.VMEM),
            scratch_shapes=[
                pltpu.VMEM((BLOCK, 32 * BLOCK), jnp.bfloat16),
                pltpu.VMEM((F0, F1), jnp.bfloat16),
                pltpu.VMEM((F1, F0), jnp.bfloat16),
                pltpu.VMEM((F2, F1), jnp.bfloat16),
                pltpu.VMEM((SLOTS, F0, PART), jnp.bfloat16),
                pltpu.VMEM((SLOTS, F0, PART), jnp.bfloat16),
                pltpu.VMEM((BLOCK, F0), jnp.float32),
                pltpu.VMEM((BLOCK, F1), jnp.float32),
                pltpu.VMEM((BLOCK, F0), jnp.float32),
                pltpu.VMEM((BLOCK, F1), jnp.float32),
                pltpu.SemaphoreType.DMA((2,)),
                pltpu.SemaphoreType.DMA((BLOCK // BAND,)),
                pltpu.SemaphoreType.DMA((3,)),
                pltpu.SemaphoreType.DMA((SLOTS,)),
                pltpu.SemaphoreType.DMA((SLOTS,)),
                pltpu.SemaphoreType.DMA((2, 3)),
                pltpu.SemaphoreType.DMA((2,)),
                pltpu.SemaphoreType.DMA((2,)),
            ],
            compiler_params=pltpu.CompilerParams(
                collective_id=0, has_side_effects=True, vmem_limit_bytes=60 * 1024 * 1024),
        )(adj, mask, h0t, w1, w2t).T

    return jax.shard_map(step, mesh=mesh, in_specs=(P('rows', 'rep'), P(), P('rows', None), P(), P()),
                         out_specs=P('rows', None), check_vma=False)
```

```python
import jax
import jax.numpy as jnp
from jax import lax
from jax.experimental import pallas as pl
from jax.experimental.pallas import tpu as pltpu
from jax.sharding import PartitionSpec as P

BLOCK = 384
F0, F1, F2 = 200, 512, 107
PART = 128
SLOTS = 96
CHUNKS = 8, 4
BAND = 32
DIRECT = 9, 9, 4
LEAD = 24
AXES = ('xyz', 'yzx', 'zxy')
MESH = pl.DeviceIdType.MESH


def relay_bit(p, axis, off):
    before = AXES[p][:AXES[p].index(axis)]
    return sum(off[a] for a in before) % 2


def piece_sends(is_src, p, zc, dy, dx):
    off = {'x': dx, 'y': dy, 'z': zc}
    order = AXES[p]
    last, depth, direct = -1, 0, []
    for i, a in enumerate(order):
        direct.append(depth >= DIRECT[i])
        steps = (zc if is_src else 1 + zc) if a == 'z' else (0, 1, 2, 1)[off[a]]
        if steps:
            last = i
            depth += 1 if direct[i] else steps
    out = []
    if last >= 0 and not direct[last]:
        a = order[last]
        bit = relay_bit(p, a, off)
        if a in 'xy':
            if off[a] == 3 and bit == 0:
                out.append((a, 1))
            if off[a] == 1 and bit == 1:
                out.append((a, -1))
        elif is_src and zc == 1 and bit == 0:
            out.append(('z', -1))
        elif not is_src and zc == 0 and bit == 1:
            out.append(('z', -1))
    for i in range(last + 1, 3):
        out += [(order[i], 1), (order[i], -1)] + [(order[i], 2)] * direct[i]
    return out


def words(codes):
    return [(c // 32, c // 16 % 2, c // 4 % 4, c % 4) for c in codes]


SRC_CODES = [
    0, 32, 64, 1, 3, 36, 44, 80, 4, 12, 48, 65, 67, 16, 33, 35, 68, 76, 2, 60, 52, 40, 7, 83,
    84, 13, 5, 81, 15, 17, 19, 37, 45, 66, 92, 8, 39, 28, 20, 49, 69, 71, 34, 79, 51, 14, 56, 77,
    82, 6, 47, 72, 18, 11, 53, 61, 41, 85, 9, 21, 23, 87, 55, 63, 93, 43, 29, 31, 95, 88, 38, 46,
    10, 70, 24, 78, 73, 75, 59, 94, 30, 50, 57, 22, 86, 25, 27, 54, 89, 62, 42, 91, 26, 74, 58, 90,
]
SINK_CODES = [
    64, 32, 0, 80, 65, 67, 44, 36, 68, 48, 76, 1, 3, 4, 12, 35, 83, 81, 92, 40, 66, 60, 52, 16,
    84, 2, 69, 45, 71, 37, 5, 33, 7, 77, 79, 13, 72, 15, 47, 39, 82, 8, 49, 17, 20, 19, 56, 51,
    34, 14, 28, 43, 95, 6, 18, 93, 41, 63, 78, 11, 55, 9, 87, 85, 61, 53, 70, 88, 73, 21, 23, 46,
    38, 75, 94, 29, 31, 59, 50, 57, 86, 30, 42, 91, 10, 24, 89, 22, 90, 62, 26, 54, 74, 25, 27, 58,
]
SRC_ORDER, SINK_ORDER = words(SRC_CODES), words(SINK_CODES)


def kernel(adj, mask_h, h0t, w1, out, a_v, mask, w1_v, w1t, tab1, tab2, y_two, acc1, acc2, peer1, peer2,
           load_sem, adj_sem, own_sem, recv_sem1, recv_sem2, send_sem, peer_send, peer_recv):
    rep = lax.axis_index('rep')
    row = lax.axis_index('rows')
    z, y, x = lax.div(row, 16), lax.rem(lax.div(row, 4), 4), lax.rem(row, 4)
    zr = lax.rem(z + 4 - 2 * rep, 4)
    is_src = zr < 2
    near = lax.div(lax.rem(zr + 1, 4), 2)
    inward = 1 - 2 * near
    xs = [lax.rem(x + d, 4) for d in range(4)]
    ys = [lax.rem(y + d, 4) for d in range(4)]
    planes = [near * 48, 48 - near * 48]
    grid = [[[planes[zc] + ys[dy] * 12 + xs[dx] * 3 for dx in range(4)] for dy in range(4)] for zc in range(2)]

    def rows_at(axis, d):
        if axis == 'x':
            return z * 16 + y * 4 + xs[d % 4]
        if axis == 'y':
            return z * 16 + ys[d % 4] * 4 + x
        return lax.rem(z + d * inward + 4, 4) * 16 + y * 4 + x

    links = [(axis, d) for axis in 'xyz' for d in (1, -1, 2)]
    target = {link: rows_at(*link) for link in links}

    barrier = pltpu.get_barrier_semaphore()
    for link in links:
        pl.semaphore_signal(barrier, inc=1, device_id=(rep, target[link]), device_id_type=MESH)
    pl.semaphore_signal(barrier, inc=1, device_id=(1 - rep, row), device_id_type=MESH)

    loads = [pltpu.make_async_copy(src, dst, load_sem.at[i]) for i, (src, dst) in enumerate([(w1, w1_v), (mask_h, mask)])]
    bands = [pl.ds(i * BAND, BAND) for i in range(BLOCK // BAND)]
    adj_loads = [pltpu.make_async_copy(adj.at[rows], a_v.at[rows], adj_sem.at[i]) for i, rows in enumerate(bands)]

    def slot_of(word):
        p, zc, dy, dx = word
        return grid[zc][dy][dx] + p

    def send_piece(layer, tab, recv_sem, src_role, word):
        slot = slot_of(word)
        for link in piece_sends(src_role, *word):
            pltpu.make_async_remote_copy(
                src_ref=tab.at[slot], dst_ref=tab.at[slot],
                send_sem=send_sem.at[layer, 'xyz'.index(link[0])], recv_sem=recv_sem.at[slot],
                device_id=(rep, target[link]), device_id_type=MESH).start()

    def wait_piece(tab, recv_sem, word):
        slot = slot_of(word)
        pltpu.make_async_copy(tab.at[slot], tab.at[slot], recv_sem.at[slot]).wait()

    own = [(p, 0, 0, 0) for p in range(3)]

    own_loads = [pltpu.make_async_copy(h0t.at[:, pl.ds(p * PART, PART)], tab1.at[slot_of(own[p])], own_sem.at[p]) for p in range(3)]

    @pl.when(is_src)
    def _():
        for copy in own_loads:
            copy.start()

    for copy in loads + adj_loads:
        copy.start()

    @pl.when(is_src)
    def _():
        for copy in own_loads:
            copy.wait()

    pl.semaphore_wait(barrier, len(links) + 1)

    @pl.when(is_src)
    def _():
        for p in range(3):
            send_piece(0, tab1, recv_sem1, True, own[p])

    loads[0].wait()
    w1t[...] = w1_v[...].astype(jnp.float32).T.astype(jnp.bfloat16)
    acc1[...] = jnp.zeros_like(acc1)
    acc2[...] = jnp.zeros_like(acc2)

    def chunk_operands(tab, first, count):
        a_parts, t_parts = [], []
        for n in range(first, first + count):
            slot = lax.select(is_src, slot_of(SRC_ORDER[n]), slot_of(SINK_ORDER[n]))
            keep = mask[row, rep * 32 + lax.div(slot, 3)].astype(jnp.float32).astype(jnp.bfloat16)
            a_parts.append(a_v[:, pl.ds(pl.multiple_of(slot * PART, PART), PART)])
            t_parts.append(tab[slot] * keep)
        return jnp.concatenate(a_parts, axis=1), jnp.concatenate(t_parts, axis=1)

    def relay(layer, tab, recv_sem, words):

        @pl.when(is_src)
        def _():
            for n in words:
                if SRC_ORDER[n] not in own:
                    wait_piece(tab, recv_sem, SRC_ORDER[n])
                    send_piece(layer, tab, recv_sem, True, SRC_ORDER[n])

        @pl.when(jnp.logical_not(is_src))
        def _():
            for n in words:
                wait_piece(tab, recv_sem, SINK_ORDER[n])
                send_piece(layer, tab, recv_sem, False, SINK_ORDER[n])

    def gather(layer, tab, recv_sem, multiply, count, lead):
        done = 0
        for first in range(0, SLOTS, count):
            relay(layer, tab, recv_sem, range(first, first + count))
            if first + count < lead:
                continue
            if layer == 0 and done == 0:
                loads[1].wait()
                for copy in adj_loads:
                    copy.wait()
            for _ in range(2):
                if done <= first:
                    multiply(*chunk_operands(tab, done, count))
                    done += count

    def multiply1(a, t):
        acc1[...] += lax.dot_general(a, t, (((1,), (1,)), ((), ())), preferred_element_type=jnp.float32)

    def multiply2(a, t):
        zt = jnp.dot(w1t[...], t, preferred_element_type=jnp.float32)
        zt = jnp.maximum(zt, 0.0).astype(jnp.bfloat16)
        acc2[...] += lax.dot_general(a, zt, (((1,), (1,)), ((), ())), preferred_element_type=jnp.float32)

    parts = [slice(p * PART, (p + 1) * PART) for p in range(3)]

    def to_peer(layer, src, dst):
        return [pltpu.make_async_remote_copy(
            src_ref=src.at[pl.ds(p * PART, PART)], dst_ref=dst.at[pl.ds(p * PART, PART)],
            send_sem=peer_send.at[layer, p], recv_sem=peer_recv.at[layer, p],
            device_id=(1 - rep, row), device_id_type=MESH) for p in range(3)]

    gather(0, tab1, recv_sem1, multiply1, CHUNKS[0], LEAD)
    swap1 = to_peer(0, acc1, peer1)

    @pl.when(jnp.logical_not(is_src))
    def _():
        for copy in swap1:
            copy.start()

    @pl.when(is_src)
    def _():
        for p in range(3):
            swap1[p].wait_recv()
            part = acc1[parts[p], :] + peer1[parts[p], :]
            tab2[slot_of(own[p])] = part.T.astype(jnp.bfloat16)
        for p in range(3):
            send_piece(1, tab2, recv_sem2, True, own[p])

    gather(1, tab2, recv_sem2, multiply2, CHUNKS[1], 0)
    swap2 = to_peer(1, acc2, peer2)
    stores = [pltpu.make_async_copy(y_two.at[pl.ds(p * PART, PART)], out.at[pl.ds(p * PART, PART)], own_sem.at[p]) for p in range(3)]
    for copy in swap2:
        copy.start()
    for p in range(3):
        swap2[p].wait_recv()
        y_two[parts[p], :] = (acc2[parts[p], :] + peer2[parts[p], :]).astype(jnp.bfloat16)
        stores[p].start()

    def drain(role):
        for layer, tab in ((0, tab1), (1, tab2)):
            for i, axis in enumerate('xyz'):
                words = SRC_ORDER if role else SINK_ORDER
                count = sum(link[0] == axis for word in words for link in piece_sends(role, *word))
                ref = tab.at[pl.ds(0, count)]
                pltpu.make_async_copy(ref, ref, send_sem.at[layer, i]).wait()

    @pl.when(is_src)
    def _():
        drain(True)

    @pl.when(jnp.logical_not(is_src))
    def _():
        drain(False)
        for copy in swap1:
            copy.wait_send()

    for copy in swap2:
        copy.wait_send()
    for copy in stores:
        copy.wait()


def solution(mesh):
    def step(adj, mask, h0, w1, w2):
        any_space = pl.BlockSpec(memory_space=pl.ANY)
        y_two = pl.pallas_call(
            kernel,
            name='gcn',
            out_shape=jax.ShapeDtypeStruct((BLOCK, F1), jnp.bfloat16),
            in_specs=[any_space] * 4,
            out_specs=any_space,
            scratch_shapes=[
                pltpu.VMEM((BLOCK, 32 * BLOCK), jnp.bfloat16),
                pltpu.SMEM((64, 64), jnp.int32),
                pltpu.VMEM((F0, F1), jnp.bfloat16),
                pltpu.VMEM((F1, F0), jnp.bfloat16),
                pltpu.VMEM((SLOTS, F0, PART), jnp.bfloat16),
                pltpu.VMEM((SLOTS, F0, PART), jnp.bfloat16),
                pltpu.VMEM((BLOCK, F1), jnp.bfloat16),
                pltpu.VMEM((BLOCK, F0), jnp.float32),
                pltpu.VMEM((BLOCK, F1), jnp.float32),
                pltpu.VMEM((BLOCK, F0), jnp.float32),
                pltpu.VMEM((BLOCK, F1), jnp.float32),
                pltpu.SemaphoreType.DMA((2,)),
                pltpu.SemaphoreType.DMA((BLOCK // BAND,)),
                pltpu.SemaphoreType.DMA((3,)),
                pltpu.SemaphoreType.DMA((SLOTS,)),
                pltpu.SemaphoreType.DMA((SLOTS,)),
                pltpu.SemaphoreType.DMA((2, 3)),
                pltpu.SemaphoreType.DMA((2, 3)),
                pltpu.SemaphoreType.DMA((2, 3)),
            ],
            compiler_params=pltpu.CompilerParams(
                collective_id=0, has_side_effects=True, vmem_limit_bytes=60 * 1024 * 1024),
        )(adj, mask, h0.T, w1)
        return jnp.dot(y_two, w2, preferred_element_type=jnp.float32)

    return jax.shard_map(step, mesh=mesh, in_specs=(P('rows', 'rep'), P(), P('rows', None), P(), P()),
                         out_specs=P('rows', None), check_vma=False)
```

```python
import jax
import jax.numpy as jnp
from jax import lax
from jax.experimental import pallas as pl
from jax.experimental.pallas import tpu as pltpu
from jax.sharding import PartitionSpec as P

BLOCK = 384
F0, F1, F2 = 200, 512, 107
PART = 128
SLOTS = 96
CHUNKS = 8, 4
BAND = 32
DIRECT = 9, 9, 4
LEAD = 24
AXES = ('xyz', 'yzx', 'zxy')
MESH = pl.DeviceIdType.MESH


def relay_bit(p, axis, off):
    before = AXES[p][:AXES[p].index(axis)]
    return sum(off[a] for a in before) % 2


def piece_sends(is_src, p, zc, dy, dx):
    off = {'x': dx, 'y': dy, 'z': zc}
    order = AXES[p]
    last, depth, direct = -1, 0, []
    for i, a in enumerate(order):
        direct.append(depth >= DIRECT[i])
        steps = (zc if is_src else 1 + zc) if a == 'z' else (0, 1, 2, 1)[off[a]]
        if steps:
            last = i
            depth += 1 if direct[i] else steps
    out = []
    if last >= 0 and not direct[last]:
        a = order[last]
        bit = relay_bit(p, a, off)
        if a in 'xy':
            if off[a] == 3 and bit == 0:
                out.append((a, 1))
            if off[a] == 1 and bit == 1:
                out.append((a, -1))
        elif is_src and zc == 1 and bit == 0:
            out.append(('z', -1))
        elif not is_src and zc == 0 and bit == 1:
            out.append(('z', -1))
    for i in range(last + 1, 3):
        out += [(order[i], 1), (order[i], -1)] + [(order[i], 2)] * direct[i]
    return out


def words(codes):
    return [(c // 32, c // 16 % 2, c // 4 % 4, c % 4) for c in codes]


SRC_CODES = [
    0, 32, 64, 3, 36, 80, 44, 4, 1, 48, 65, 67, 33, 35, 68, 76, 12, 2, 52, 40, 84, 7, 83, 81,
    60, 13, 5, 15, 16, 17, 37, 45, 66, 92, 8, 39, 20, 49, 69, 18, 71, 19, 34, 79, 51, 14, 11, 56,
    6, 77, 82, 47, 53, 61, 72, 28, 41, 85, 9, 55, 23, 21, 87, 63, 93, 43, 46, 29, 31, 95, 88, 38,
    10, 70, 24, 59, 78, 73, 57, 30, 50, 22, 75, 86, 54, 62, 42, 26, 25, 89, 91, 74, 94, 58, 27, 90,
]
SINK_CODES = [
    32, 64, 0, 80, 65, 44, 36, 3, 68, 67, 48, 76, 1, 4, 12, 35, 2, 81, 92, 40, 83, 60, 84, 69,
    45, 16, 52, 66, 71, 5, 37, 33, 7, 15, 77, 79, 13, 72, 49, 82, 17, 39, 47, 56, 51, 43, 8, 34,
    28, 14, 95, 6, 63, 93, 20, 41, 78, 55, 11, 19, 9, 87, 85, 53, 70, 21, 23, 73, 88, 18, 46, 38,
    86, 75, 94, 31, 29, 10, 59, 50, 57, 61, 30, 91, 24, 42, 89, 22, 62, 90, 26, 54, 74, 25, 27, 58,
]
SRC_ORDER, SINK_ORDER = words(SRC_CODES), words(SINK_CODES)


def kernel(adj, mask_h, h0t, w1, y_two, a_v, mask, w1_v, w1t, tab1, tab2, acc1, acc2, peer1, peer2,
           load_sem, adj_sem, own_sem, recv_sem1, recv_sem2, send_sem, peer_send, peer_recv):
    rep = lax.axis_index('rep')
    row = lax.axis_index('rows')
    z, y, x = lax.div(row, 16), lax.rem(lax.div(row, 4), 4), lax.rem(row, 4)
    zr = lax.rem(z + 4 - 2 * rep, 4)
    is_src = zr < 2
    near = lax.div(lax.rem(zr + 1, 4), 2)
    inward = 1 - 2 * near
    xs = [lax.rem(x + d, 4) for d in range(4)]
    ys = [lax.rem(y + d, 4) for d in range(4)]
    planes = [near * 48, 48 - near * 48]
    grid = [[[planes[zc] + ys[dy] * 12 + xs[dx] * 3 for dx in range(4)] for dy in range(4)] for zc in range(2)]

    def rows_at(axis, d):
        if axis == 'x':
            return z * 16 + y * 4 + xs[d % 4]
        if axis == 'y':
            return z * 16 + ys[d % 4] * 4 + x
        return lax.rem(z + d * inward + 4, 4) * 16 + y * 4 + x

    links = [(axis, d) for axis in 'xyz' for d in (1, -1, 2)]
    target = {link: rows_at(*link) for link in links}

    barrier = pltpu.get_barrier_semaphore()
    for link in links:
        pl.semaphore_signal(barrier, inc=1, device_id=(rep, target[link]), device_id_type=MESH)
    pl.semaphore_signal(barrier, inc=1, device_id=(1 - rep, row), device_id_type=MESH)

    loads = [pltpu.make_async_copy(src, dst, load_sem.at[i]) for i, (src, dst) in enumerate([(w1, w1_v), (mask_h, mask)])]
    bands = [pl.ds(i * BAND, BAND) for i in range(BLOCK // BAND)]
    adj_loads = [pltpu.make_async_copy(adj.at[rows], a_v.at[rows], adj_sem.at[i]) for i, rows in enumerate(bands)]

    def slot_of(word):
        p, zc, dy, dx = word
        return grid[zc][dy][dx] + p

    def send_piece(layer, tab, recv_sem, src_role, word):
        slot = slot_of(word)
        for link in piece_sends(src_role, *word):
            pltpu.make_async_remote_copy(
                src_ref=tab.at[slot], dst_ref=tab.at[slot],
                send_sem=send_sem.at[layer, 'xyz'.index(link[0])], recv_sem=recv_sem.at[slot],
                device_id=(rep, target[link]), device_id_type=MESH).start()

    def wait_piece(tab, recv_sem, word):
        slot = slot_of(word)
        pltpu.make_async_copy(tab.at[slot], tab.at[slot], recv_sem.at[slot]).wait()

    own = [(p, 0, 0, 0) for p in range(3)]

    own_loads = [pltpu.make_async_copy(h0t.at[:, pl.ds(p * PART, PART)], tab1.at[slot_of(own[p])], own_sem.at[p]) for p in range(3)]

    @pl.when(is_src)
    def _():
        for copy in own_loads:
            copy.start()

    for copy in loads + adj_loads:
        copy.start()

    @pl.when(is_src)
    def _():
        for copy in own_loads:
            copy.wait()

    pl.semaphore_wait(barrier, len(links) + 1)

    @pl.when(is_src)
    def _():
        for p in range(3):
            send_piece(0, tab1, recv_sem1, True, own[p])

    loads[0].wait()
    w1t[...] = w1_v[...].astype(jnp.float32).T.astype(jnp.bfloat16)
    acc1[...] = jnp.zeros_like(acc1)
    acc2[...] = jnp.zeros_like(acc2)

    def chunk_operands(tab, first, count):
        a_parts, t_parts = [], []
        for n in range(first, first + count):
            slot = lax.select(is_src, slot_of(SRC_ORDER[n]), slot_of(SINK_ORDER[n]))
            keep = mask[row, rep * 32 + lax.div(slot, 3)].astype(jnp.float32).astype(jnp.bfloat16)
            a_parts.append(a_v[:, pl.ds(pl.multiple_of(slot * PART, PART), PART)])
            t_parts.append(tab[slot] * keep)
        return jnp.concatenate(a_parts, axis=1), jnp.concatenate(t_parts, axis=1)

    def relay(layer, tab, recv_sem, words):

        @pl.when(is_src)
        def _():
            for n in words:
                if SRC_ORDER[n] not in own:
                    wait_piece(tab, recv_sem, SRC_ORDER[n])
                    send_piece(layer, tab, recv_sem, True, SRC_ORDER[n])

        @pl.when(jnp.logical_not(is_src))
        def _():
            for n in words:
                wait_piece(tab, recv_sem, SINK_ORDER[n])
                send_piece(layer, tab, recv_sem, False, SINK_ORDER[n])

    def gather(layer, tab, recv_sem, multiply, count, lead):
        done = 0
        for first in range(0, SLOTS, count):
            relay(layer, tab, recv_sem, range(first, first + count))
            if first + count < lead:
                continue
            if layer == 0 and done == 0:
                loads[1].wait()
                for copy in adj_loads:
                    copy.wait()
            for _ in range(2):
                if done <= first:
                    multiply(*chunk_operands(tab, done, count))
                    done += count

    def multiply1(a, t):
        acc1[...] += lax.dot_general(a, t, (((1,), (1,)), ((), ())), preferred_element_type=jnp.float32)

    def multiply2(a, t):
        zt = jnp.dot(w1t[...], t, preferred_element_type=jnp.float32)
        zt = jnp.maximum(zt, 0.0).astype(jnp.bfloat16)
        acc2[...] += lax.dot_general(a, zt, (((1,), (1,)), ((), ())), preferred_element_type=jnp.float32)

    parts = [slice(p * PART, (p + 1) * PART) for p in range(3)]

    def to_peer(layer, src, dst):
        return [pltpu.make_async_remote_copy(
            src_ref=src.at[pl.ds(p * PART, PART)], dst_ref=dst.at[pl.ds(p * PART, PART)],
            send_sem=peer_send.at[layer, p], recv_sem=peer_recv.at[layer, p],
            device_id=(1 - rep, row), device_id_type=MESH) for p in range(3)]

    gather(0, tab1, recv_sem1, multiply1, CHUNKS[0], LEAD)
    swap1 = to_peer(0, acc1, peer1)

    @pl.when(jnp.logical_not(is_src))
    def _():
        for copy in swap1:
            copy.start()

    @pl.when(is_src)
    def _():
        for p in range(3):
            swap1[p].wait_recv()
            part = acc1[parts[p], :] + peer1[parts[p], :]
            tab2[slot_of(own[p])] = part.T.astype(jnp.bfloat16)
        for p in range(3):
            send_piece(1, tab2, recv_sem2, True, own[p])

    gather(1, tab2, recv_sem2, multiply2, CHUNKS[1], 0)
    swap2 = to_peer(1, acc2, peer2)
    for copy in swap2:
        copy.start()
    for p in range(3):
        swap2[p].wait_recv()
        y_two[parts[p], :] = (acc2[parts[p], :] + peer2[parts[p], :]).astype(jnp.bfloat16)

    def drain(role):
        for layer, tab in ((0, tab1), (1, tab2)):
            for i, axis in enumerate('xyz'):
                words = SRC_ORDER if role else SINK_ORDER
                count = sum(link[0] == axis for word in words for link in piece_sends(role, *word))
                ref = tab.at[pl.ds(0, count)]
                pltpu.make_async_copy(ref, ref, send_sem.at[layer, i]).wait()

    @pl.when(is_src)
    def _():
        drain(True)

    @pl.when(jnp.logical_not(is_src))
    def _():
        drain(False)
        for copy in swap1:
            copy.wait_send()

    for copy in swap2:
        copy.wait_send()


def solution(mesh):
    def step(adj, mask, h0, w1, w2):
        hbm = pl.BlockSpec(memory_space=pltpu.HBM)
        y_two = pl.pallas_call(
            kernel,
            name='gcn',
            out_shape=jax.ShapeDtypeStruct((BLOCK, F1), jnp.bfloat16),
            in_specs=[hbm] * 4,
            out_specs=pl.BlockSpec(memory_space=pltpu.VMEM),
            scratch_shapes=[
                pltpu.VMEM((BLOCK, 32 * BLOCK), jnp.bfloat16),
                pltpu.SMEM((64, 64), jnp.int32),
                pltpu.VMEM((F0, F1), jnp.bfloat16),
                pltpu.VMEM((F1, F0), jnp.bfloat16),
                pltpu.VMEM((SLOTS, F0, PART), jnp.bfloat16),
                pltpu.VMEM((SLOTS, F0, PART), jnp.bfloat16),
                pltpu.VMEM((BLOCK, F0), jnp.float32),
                pltpu.VMEM((BLOCK, F1), jnp.float32),
                pltpu.VMEM((BLOCK, F0), jnp.float32),
                pltpu.VMEM((BLOCK, F1), jnp.float32),
                pltpu.SemaphoreType.DMA((2,)),
                pltpu.SemaphoreType.DMA((BLOCK // BAND,)),
                pltpu.SemaphoreType.DMA((3,)),
                pltpu.SemaphoreType.DMA((SLOTS,)),
                pltpu.SemaphoreType.DMA((SLOTS,)),
                pltpu.SemaphoreType.DMA((2, 3)),
                pltpu.SemaphoreType.DMA((2, 3)),
                pltpu.SemaphoreType.DMA((2, 3)),
            ],
            compiler_params=pltpu.CompilerParams(
                collective_id=0, has_side_effects=True, vmem_limit_bytes=40 * 1024 * 1024),
        )(*[pltpu.with_memory_space_constraint(a, pltpu.HBM) for a in (adj, mask, h0.T, w1)])
        return jnp.dot(y_two, w2, preferred_element_type=jnp.float32)

    return jax.shard_map(step, mesh=mesh, in_specs=(P('rows', 'rep'), P(), P('rows', None), P(), P()),
                         out_specs=P('rows', None), check_vma=False)
```

```python
import jax
import jax.numpy as jnp
from jax import lax
from jax.experimental import pallas as pl
from jax.experimental.pallas import tpu as pltpu
from jax.sharding import PartitionSpec as P

BLOCK = 384
F0, F1, F2 = 200, 512, 107
PART = 128
SLOTS = 96
CHUNKS = 8, 4
BAND = 32
DIRECT = (9, 9, 4), (9, 9, 4)
LEAD = 3
AXES = ('xyz', 'yzx', 'zxy')
MESH = pl.DeviceIdType.MESH


def relay_bit(p, axis, off):
    before = AXES[p][:AXES[p].index(axis)]
    return sum(off[a] for a in before) % 2


def piece_sends(layer, is_src, p, zc, dy, dx):
    off = {'x': dx, 'y': dy, 'z': zc}
    order = AXES[p]
    last, depth, direct = -1, 0, []
    for i, a in enumerate(order):
        direct.append(depth >= DIRECT[layer][i])
        steps = (zc if is_src else 1 + zc) if a == 'z' else (0, 1, 2, 1)[off[a]]
        if steps:
            last = i
            depth += 1 if direct[i] else steps
    out = []
    if last >= 0 and not direct[last]:
        a = order[last]
        bit = relay_bit(p, a, off)
        if a in 'xy':
            if off[a] == 3 and bit == 0:
                out.append((a, 1))
            if off[a] == 1 and bit == 1:
                out.append((a, -1))
        elif is_src and zc == 1 and bit == 0:
            out.append(('z', -1))
        elif not is_src and zc == 0 and bit == 1:
            out.append(('z', -1))
    for i in range(last + 1, 3):
        out += [(order[i], 1), (order[i], -1)] + [(order[i], 2)] * direct[i]
    return out


ORDER_CODES = [
    [32, 3136, 6224, 420, 353, 3500, 7747, 4292, 3216, 4684, 100, 6240, 6467, 6529, 3372, 7377, 1192, 195, 4994, 3900, 756, 8060, 1331, 7845,
     1485, 8080, 532, 1602, 8903, 5765, 4357, 3777, 1639, 6387, 4781, 847, 3591, 6673, 6888, 1745, 1967, 3298, 4952, 1906, 1387, 7598, 5471, 591,
     1069, 4532, 6920, 3964, 7878, 7455, 5897, 3069, 949, 2743, 5358, 4427, 8947, 5163, 2025, 2278, 8425, 6101, 2830, 6807, 9208, 8178, 8498, 3671,
     5694, 4222, 1019, 2325, 5503, 7549, 2141, 7238, 8347, 2966, 4842, 5962, 2457, 4054, 8633, 2558, 8760, 9051, 5622, 2650, 5274, 7178, 8665, 7034],
    [0, 3104, 6208, 368, 161, 3500, 7716, 452, 4291, 6241, 4656, 7331, 1228, 3249, 676, 6444, 4997, 225, 8147, 3363, 520, 1692, 7868, 1293,
     1989, 3892, 1583, 6413, 4357, 6823, 1506, 783, 5839, 8848, 7981, 6626, 6545, 1908, 3624, 1415, 1779, 7921, 3278, 7666, 1067, 5415, 632, 7426,
     8491, 4724, 3752, 4607, 8166, 949, 4924, 5151, 2249, 5949, 6967, 5367, 4489, 2766, 2025, 8371, 8981, 6118, 2872, 4149, 3022, 7511, 7275, 9158,
     7037, 978, 6781, 2930, 3734, 3967, 2363, 5758, 2410, 8298, 5502, 4857, 5246, 6043, 9051, 2134, 7158, 2585, 2616, 4057, 8570, 8826, 8698, 5642],
]


def words(codes):
    return [(c // 32, c // 16 % 2, c // 4 % 4, c % 4) for c in codes]


SRC_ORDER = [words([c // SLOTS for c in codes]) for codes in ORDER_CODES]
SINK_ORDER = [words([c % SLOTS for c in codes]) for codes in ORDER_CODES]


def kernel(adj, mask_h, h0t, w1, y_two, a_v, mask, w1_v, w1t, tab1, tab2, acc1, acc2, peer1, peer2,
           load_sem, adj_sem, own_sem, recv_sem1, recv_sem2, send_sem, peer_send, peer_recv):
    rep = lax.axis_index('rep')
    row = lax.axis_index('rows')
    z, y, x = lax.div(row, 16), lax.rem(lax.div(row, 4), 4), lax.rem(row, 4)
    zr = lax.rem(z + 4 - 2 * rep, 4)
    is_src = zr < 2
    near = lax.div(lax.rem(zr + 1, 4), 2)
    inward = 1 - 2 * near
    xs = [lax.rem(x + d, 4) for d in range(4)]
    ys = [lax.rem(y + d, 4) for d in range(4)]
    planes = [near * 48, 48 - near * 48]
    grid = [[[planes[zc] + ys[dy] * 12 + xs[dx] * 3 for dx in range(4)] for dy in range(4)] for zc in range(2)]

    def rows_at(axis, d):
        if axis == 'x':
            return z * 16 + y * 4 + xs[d % 4]
        if axis == 'y':
            return z * 16 + ys[d % 4] * 4 + x
        return lax.rem(z + d * inward + 4, 4) * 16 + y * 4 + x

    links = [(axis, d) for axis in 'xyz' for d in (1, -1, 2)]
    target = {link: rows_at(*link) for link in links}

    loads = [pltpu.make_async_copy(src, dst, load_sem.at[i]) for i, (src, dst) in enumerate([(w1, w1_v), (mask_h, mask)])]
    bands = [pl.ds(i * BAND, BAND) for i in range(BLOCK // BAND)]
    adj_loads = [pltpu.make_async_copy(adj.at[rows], a_v.at[rows], adj_sem.at[i]) for i, rows in enumerate(bands)]

    def slot_of(word):
        p, zc, dy, dx = word
        return grid[zc][dy][dx] + p

    def send_piece(layer, tab, recv_sem, src_role, word):
        slot = slot_of(word)
        for link in piece_sends(layer, src_role, *word):
            pltpu.make_async_remote_copy(
                src_ref=tab.at[slot], dst_ref=tab.at[slot],
                send_sem=send_sem.at[layer, 'xyz'.index(link[0])], recv_sem=recv_sem.at[slot],
                device_id=(rep, target[link]), device_id_type=MESH).start()

    def wait_piece(tab, recv_sem, word):
        slot = slot_of(word)
        pltpu.make_async_copy(tab.at[slot], tab.at[slot], recv_sem.at[slot]).wait()

    own = [(p, 0, 0, 0) for p in range(3)]

    own_loads = [pltpu.make_async_copy(h0t.at[:, pl.ds(p * PART, PART)], tab1.at[slot_of(own[p])], own_sem.at[p]) for p in range(3)]

    @pl.when(is_src)
    def _():
        for copy in own_loads:
            copy.start()

    barrier = pltpu.get_barrier_semaphore()
    for link in links:
        pl.semaphore_signal(barrier, inc=1, device_id=(rep, target[link]), device_id_type=MESH)
    pl.semaphore_signal(barrier, inc=1, device_id=(1 - rep, row), device_id_type=MESH)

    for copy in loads + adj_loads:
        copy.start()

    @pl.when(is_src)
    def _():
        for copy in own_loads:
            copy.wait()

    pl.semaphore_wait(barrier, len(links) + 1)

    @pl.when(is_src)
    def _():
        for p in range(3):
            send_piece(0, tab1, recv_sem1, True, own[p])

    loads[0].wait()
    w1t[...] = w1_v[...].astype(jnp.float32).T.astype(jnp.bfloat16)
    acc1[...] = jnp.zeros_like(acc1)
    acc2[...] = jnp.zeros_like(acc2)

    def chunk_operands(layer, tab, first, count):
        a_parts, t_parts = [], []
        for n in range(first, first + count):
            slot = lax.select(is_src, slot_of(SRC_ORDER[layer][n]), slot_of(SINK_ORDER[layer][n]))
            keep = mask[row, rep * 32 + lax.div(slot, 3)].astype(jnp.float32).astype(jnp.bfloat16)
            a_parts.append(a_v[:, pl.ds(pl.multiple_of(slot * PART, PART), PART)])
            t_parts.append(tab[slot] * keep)
        return jnp.concatenate(a_parts, axis=1), jnp.concatenate(t_parts, axis=1)

    def relay(layer, tab, recv_sem, words):

        @pl.when(is_src)
        def _():
            for n in words:
                if SRC_ORDER[layer][n] not in own:
                    wait_piece(tab, recv_sem, SRC_ORDER[layer][n])
                    send_piece(layer, tab, recv_sem, True, SRC_ORDER[layer][n])

        @pl.when(jnp.logical_not(is_src))
        def _():
            for n in words:
                wait_piece(tab, recv_sem, SINK_ORDER[layer][n])
                send_piece(layer, tab, recv_sem, False, SINK_ORDER[layer][n])

    def gather(layer, tab, recv_sem, multiply, size, lead):
        bounds = [(first, size) for first in range(0, SLOTS - size, size)]
        bounds += [(SLOTS - size, size // 2), (SLOTS - size // 2, size // 2)]
        todo = []
        for i, (first, count) in enumerate(bounds):
            relay(layer, tab, recv_sem, range(first, first + count))
            todo.append((first, count))
            if i + 1 < lead:
                continue
            if layer == 0 and i + 1 == lead:
                loads[1].wait()
                for copy in adj_loads:
                    copy.wait()
            for chunk in todo[:2]:
                multiply(*chunk_operands(layer, tab, *chunk))
            todo = todo[2:]
        assert not todo

    def multiply1(a, t):
        acc1[:, :F0] += lax.dot_general(a, t, (((1,), (1,)), ((), ())), preferred_element_type=jnp.float32)

    def multiply2(a, t):
        zt = jnp.dot(w1t[...], t, preferred_element_type=jnp.float32)
        zt = jnp.maximum(zt, 0.0).astype(jnp.bfloat16)
        acc2[...] += lax.dot_general(a, zt, (((1,), (1,)), ((), ())), preferred_element_type=jnp.float32)

    parts = [slice(p * PART, (p + 1) * PART) for p in range(3)]

    def to_peer(layer, src, dst):
        return [pltpu.make_async_remote_copy(
            src_ref=src.at[pl.ds(p * PART, PART)], dst_ref=dst.at[pl.ds(p * PART, PART)],
            send_sem=peer_send.at[layer, p], recv_sem=peer_recv.at[layer, p],
            device_id=(1 - rep, row), device_id_type=MESH) for p in range(3)]

    gather(0, tab1, recv_sem1, multiply1, CHUNKS[0], LEAD)
    swap1 = to_peer(0, acc1, peer1)

    @pl.when(jnp.logical_not(is_src))
    def _():
        for copy in swap1:
            copy.start()

    @pl.when(is_src)
    def _():
        for p in range(3):
            swap1[p].wait_recv()
            part = acc1[parts[p], :F0] + peer1[parts[p], :F0]
            tab2[slot_of(own[p])] = part.T.astype(jnp.bfloat16)
        for p in range(3):
            send_piece(1, tab2, recv_sem2, True, own[p])

    gather(1, tab2, recv_sem2, multiply2, CHUNKS[1], 1)
    swap2 = to_peer(1, acc2, peer2)
    for copy in swap2:
        copy.start()
    for p in range(3):
        swap2[p].wait_recv()
        y_two[parts[p], :] = (acc2[parts[p], :] + peer2[parts[p], :]).astype(jnp.bfloat16)

    def drain(role):
        for layer, tab in ((0, tab1), (1, tab2)):
            for i, axis in enumerate('xyz'):
                words = SRC_ORDER[layer] if role else SINK_ORDER[layer]
                count = sum(link[0] == axis for word in words for link in piece_sends(layer, role, *word))
                ref = tab.at[pl.ds(0, count)]
                pltpu.make_async_copy(ref, ref, send_sem.at[layer, i]).wait()

    @pl.when(is_src)
    def _():
        drain(True)

    @pl.when(jnp.logical_not(is_src))
    def _():
        drain(False)
        for copy in swap1:
            copy.wait_send()

    for copy in swap2:
        copy.wait_send()


def solution(mesh):
    def step(adj, mask, h0, w1, w2):
        hbm = pl.BlockSpec(memory_space=pltpu.HBM)
        y_two = pl.pallas_call(
            kernel,
            name='gcn',
            out_shape=jax.ShapeDtypeStruct((BLOCK, F1), jnp.bfloat16),
            in_specs=[hbm] * 4,
            out_specs=pl.BlockSpec(memory_space=pltpu.VMEM),
            scratch_shapes=[
                pltpu.VMEM((BLOCK, 32 * BLOCK), jnp.bfloat16),
                pltpu.SMEM((64, 64), jnp.int32),
                pltpu.VMEM((F0, F1), jnp.bfloat16),
                pltpu.VMEM((F1, F0), jnp.bfloat16),
                pltpu.VMEM((SLOTS, F0, PART), jnp.bfloat16),
                pltpu.VMEM((SLOTS, F0, PART), jnp.bfloat16),
                pltpu.VMEM((BLOCK, 256), jnp.float32),
                pltpu.VMEM((BLOCK, F1), jnp.float32),
                pltpu.VMEM((BLOCK, 256), jnp.float32),
                pltpu.VMEM((BLOCK, F1), jnp.float32),
                pltpu.SemaphoreType.DMA((2,)),
                pltpu.SemaphoreType.DMA((BLOCK // BAND,)),
                pltpu.SemaphoreType.DMA((3,)),
                pltpu.SemaphoreType.DMA((SLOTS,)),
                pltpu.SemaphoreType.DMA((SLOTS,)),
                pltpu.SemaphoreType.DMA((2, 3)),
                pltpu.SemaphoreType.DMA((2, 3)),
                pltpu.SemaphoreType.DMA((2, 3)),
            ],
            compiler_params=pltpu.CompilerParams(
                collective_id=0, has_side_effects=True, vmem_limit_bytes=40 * 1024 * 1024),
        )(*[pltpu.with_memory_space_constraint(a, pltpu.HBM) for a in (adj, mask, h0.T, w1)])
        return jnp.dot(y_two, w2, preferred_element_type=jnp.float32)

    return jax.shard_map(step, mesh=mesh, in_specs=(P('rows', 'rep'), P(), P('rows', None), P(), P()),
                         out_specs=P('rows', None), check_vma=False)
```

```python
import jax
import jax.numpy as jnp
from jax import lax
from jax.experimental import pallas as pl
from jax.experimental.pallas import tpu as pltpu
from jax.sharding import PartitionSpec as P

BLOCK = 384
F0, F1, F2 = 200, 512, 107
PART = 128
SLOTS = 96
CHUNKS = 8, 4
BAND = 32
DIRECT = (9, 9, 4), (9, 9, 4)
LEAD = 3
AXES = ('xyz', 'yzx', 'zxy')
MESH = pl.DeviceIdType.MESH


def relay_bit(p, axis, off):
    before = AXES[p][:AXES[p].index(axis)]
    return sum(off[a] for a in before) % 2


def piece_sends(layer, is_src, p, zc, dy, dx):
    off = {'x': dx, 'y': dy, 'z': zc}
    order = AXES[p]
    last, depth, direct = -1, 0, []
    for i, a in enumerate(order):
        direct.append(depth >= DIRECT[layer][i])
        steps = (zc if is_src else 1 + zc) if a == 'z' else (0, 1, 2, 1)[off[a]]
        if steps:
            last = i
            depth += 1 if direct[i] else steps
    out = []
    if last >= 0 and not direct[last]:
        a = order[last]
        bit = relay_bit(p, a, off)
        if a in 'xy':
            if off[a] == 3 and bit == 0:
                out.append((a, 1))
            if off[a] == 1 and bit == 1:
                out.append((a, -1))
        elif is_src and zc == 1 and bit == 0:
            out.append(('z', -1))
        elif not is_src and zc == 0 and bit == 1:
            out.append(('z', -1))
    for i in range(last + 1, 3):
        out += [(order[i], 1), (order[i], -1)] + [(order[i], 2)] * direct[i]
    return out


ORDER_CODES = [
    [32, 3136, 6224, 420, 353, 3500, 7747, 4292, 3216, 4684, 100, 6240, 6467, 6529, 3372, 7377, 1192, 195, 4994, 3900, 756, 8060, 1331, 7845,
     1485, 8080, 532, 1602, 8903, 5765, 4357, 3777, 1639, 6387, 4781, 847, 3591, 6673, 6888, 1745, 1967, 3298, 4952, 1906, 1387, 7598, 5471, 591,
     1069, 4532, 6920, 3964, 7878, 7455, 5897, 3069, 949, 2743, 5358, 4427, 8947, 5163, 2025, 2278, 8425, 6101, 2830, 6807, 9208, 8178, 8498, 3671,
     5694, 4222, 1019, 2325, 5503, 7549, 2141, 7238, 8347, 2966, 4842, 5962, 2457, 4054, 8633, 2558, 8760, 9051, 5622, 2650, 5274, 7178, 8665, 7034],
    [0, 3104, 6208, 368, 161, 3500, 7716, 452, 4291, 6241, 4656, 7331, 1228, 3249, 676, 6444, 4997, 225, 8147, 3363, 520, 1692, 7868, 1293,
     1989, 3892, 1583, 6413, 4357, 6823, 1506, 783, 5839, 8848, 7981, 6626, 6545, 1908, 3624, 1415, 1779, 7921, 3278, 7666, 1067, 5415, 632, 7426,
     8491, 4724, 3752, 4607, 8166, 949, 4924, 5151, 2249, 5949, 6967, 5367, 4489, 2766, 2025, 8371, 8981, 6118, 2872, 4149, 3022, 7511, 7275, 9158,
     7037, 978, 6781, 2930, 3734, 3967, 2363, 5758, 2410, 8298, 5502, 4857, 5246, 6043, 9051, 2134, 7158, 2585, 2616, 4057, 8570, 8826, 8698, 5642],
]


def words(codes):
    return [(c // 32, c // 16 % 2, c // 4 % 4, c % 4) for c in codes]


SRC_ORDER = [words([c // SLOTS for c in codes]) for codes in ORDER_CODES]
SINK_ORDER = [words([c % SLOTS for c in codes]) for codes in ORDER_CODES]


def kernel(adj, mask_h, h0t, w1, y_two, a_v, mask, w1_v, w1t, tab1, tab2, acc1, acc2, peer1, peer2,
           load_sem, adj_sem, own_sem, recv_sem1, recv_sem2, send_sem, peer_send, peer_recv):
    rep = lax.axis_index('rep')
    row = lax.axis_index('rows')
    z, y, x = lax.div(row, 16), lax.rem(lax.div(row, 4), 4), lax.rem(row, 4)
    zr = lax.rem(z + 4 - 2 * rep, 4)
    is_src = zr < 2
    near = lax.div(lax.rem(zr + 1, 4), 2)
    inward = 1 - 2 * near
    xs = [lax.rem(x + d, 4) for d in range(4)]
    ys = [lax.rem(y + d, 4) for d in range(4)]
    planes = [near * 48, 48 - near * 48]
    grid = [[[planes[zc] + ys[dy] * 12 + xs[dx] * 3 for dx in range(4)] for dy in range(4)] for zc in range(2)]

    def rows_at(axis, d):
        if axis == 'x':
            return z * 16 + y * 4 + xs[d % 4]
        if axis == 'y':
            return z * 16 + ys[d % 4] * 4 + x
        return lax.rem(z + d * inward + 4, 4) * 16 + y * 4 + x

    links = [(axis, d) for axis in 'xyz' for d in (1, -1, 2)]
    target = {link: rows_at(*link) for link in links}

    loads = [pltpu.make_async_copy(src, dst, load_sem.at[i]) for i, (src, dst) in enumerate([(w1, w1_v), (mask_h, mask)])]
    bands = [pl.ds(i * BAND, BAND) for i in range(BLOCK // BAND)]
    adj_loads = [pltpu.make_async_copy(adj.at[rows], a_v.at[rows], adj_sem.at[i]) for i, rows in enumerate(bands)]

    def slot_of(word):
        p, zc, dy, dx = word
        return grid[zc][dy][dx] + p

    def send_piece(layer, tab, recv_sem, src_role, word):
        slot = slot_of(word)
        for link in piece_sends(layer, src_role, *word):
            pltpu.make_async_remote_copy(
                src_ref=tab.at[slot], dst_ref=tab.at[slot],
                send_sem=send_sem.at[layer, 'xyz'.index(link[0])], recv_sem=recv_sem.at[slot],
                device_id=(rep, target[link]), device_id_type=MESH).start()

    def wait_piece(tab, recv_sem, word):
        slot = slot_of(word)
        pltpu.make_async_copy(tab.at[slot], tab.at[slot], recv_sem.at[slot]).wait()

    own = [(p, 0, 0, 0) for p in range(3)]

    own_loads = [pltpu.make_async_copy(h0t.at[:, pl.ds(p * PART, PART)], tab1.at[slot_of(own[p])], own_sem.at[p]) for p in range(3)]

    @pl.when(is_src)
    def _():
        for copy in own_loads:
            copy.start()

    barrier = pltpu.get_barrier_semaphore()
    for link in links:
        pl.semaphore_signal(barrier, inc=1, device_id=(rep, target[link]), device_id_type=MESH)
    pl.semaphore_signal(barrier, inc=1, device_id=(1 - rep, row), device_id_type=MESH)

    for copy in loads + adj_loads:
        copy.start()

    @pl.when(is_src)
    def _():
        for copy in own_loads:
            copy.wait()

    pl.semaphore_wait(barrier, len(links) + 1)

    @pl.when(is_src)
    def _():
        for p in range(3):
            send_piece(0, tab1, recv_sem1, True, own[p])

    loads[0].wait()
    w1t[...] = w1_v[...].astype(jnp.float32).T.astype(jnp.bfloat16)
    acc1[...] = jnp.zeros_like(acc1)
    acc2[...] = jnp.zeros_like(acc2)

    def chunk_operands(layer, tab, first, count):
        a_parts, t_parts = [], []
        for n in range(first, first + count):
            slot = lax.select(is_src, slot_of(SRC_ORDER[layer][n]), slot_of(SINK_ORDER[layer][n]))
            keep = mask[row, rep * 32 + lax.div(slot, 3)].astype(jnp.float32).astype(jnp.bfloat16)
            a_parts.append(a_v[:, pl.ds(pl.multiple_of(slot * PART, PART), PART)])
            t_parts.append(tab[slot] * keep)
        return jnp.concatenate(a_parts, axis=1), jnp.concatenate(t_parts, axis=1)

    def relay(layer, tab, recv_sem, words):

        @pl.when(is_src)
        def _():
            for n in words:
                if SRC_ORDER[layer][n] not in own:
                    wait_piece(tab, recv_sem, SRC_ORDER[layer][n])
                    send_piece(layer, tab, recv_sem, True, SRC_ORDER[layer][n])

        @pl.when(jnp.logical_not(is_src))
        def _():
            for n in words:
                wait_piece(tab, recv_sem, SINK_ORDER[layer][n])
                send_piece(layer, tab, recv_sem, False, SINK_ORDER[layer][n])

    def gather(layer, tab, recv_sem, multiply, size, lead):
        bounds = [(first, size) for first in range(0, SLOTS - size, size)]
        bounds += [(SLOTS - size, size // 2), (SLOTS - size // 2, size // 2)]
        todo = []
        for i, (first, count) in enumerate(bounds):
            relay(layer, tab, recv_sem, range(first, first + count))
            todo.append((first, count))
            if i + 1 < lead:
                continue
            if layer == 0 and i + 1 == lead:
                loads[1].wait()
                for copy in adj_loads:
                    copy.wait()
            for chunk in todo[:2]:
                multiply(*chunk_operands(layer, tab, *chunk))
            todo = todo[2:]
        assert not todo

    def multiply1(a, t):
        acc1[:, :F0] += lax.dot_general(a, t, (((1,), (1,)), ((), ())), preferred_element_type=jnp.float32)

    def multiply2(a, t):
        zt = jnp.dot(w1t[...], t, preferred_element_type=jnp.float32)
        zt = jnp.maximum(zt, 0.0).astype(jnp.bfloat16)
        acc2[...] += lax.dot_general(a, zt, (((1,), (1,)), ((), ())), preferred_element_type=jnp.float32)

    parts = [slice(p * PART, (p + 1) * PART) for p in range(3)]

    def to_peer(layer, src, dst):
        return [pltpu.make_async_remote_copy(
            src_ref=src.at[pl.ds(p * PART, PART)], dst_ref=dst.at[pl.ds(p * PART, PART)],
            send_sem=peer_send.at[layer, p], recv_sem=peer_recv.at[layer, p],
            device_id=(1 - rep, row), device_id_type=MESH) for p in range(3)]

    gather(0, tab1, recv_sem1, multiply1, CHUNKS[0], LEAD)
    swap1 = to_peer(0, acc1, peer1)

    @pl.when(jnp.logical_not(is_src))
    def _():
        for copy in swap1:
            copy.start()

    @pl.when(is_src)
    def _():
        for p in range(3):
            swap1[p].wait_recv()
            part = acc1[parts[p], :F0] + peer1[parts[p], :F0]
            tab2[slot_of(own[p])] = part.T.astype(jnp.bfloat16)
            if p:
                send_piece(1, tab2, recv_sem2, True, own[p - 1])
        send_piece(1, tab2, recv_sem2, True, own[2])

    gather(1, tab2, recv_sem2, multiply2, CHUNKS[1], 1)
    swap2 = to_peer(1, acc2, peer2)
    for copy in swap2:
        copy.start()
    for p in range(3):
        swap2[p].wait_recv()
        y_two[parts[p], :] = (acc2[parts[p], :] + peer2[parts[p], :]).astype(jnp.bfloat16)

    def drain(role):
        for layer, tab in ((0, tab1), (1, tab2)):
            for i, axis in enumerate('xyz'):
                words = SRC_ORDER[layer] if role else SINK_ORDER[layer]
                count = sum(link[0] == axis for word in words for link in piece_sends(layer, role, *word))
                ref = tab.at[pl.ds(0, count)]
                pltpu.make_async_copy(ref, ref, send_sem.at[layer, i]).wait()

    @pl.when(is_src)
    def _():
        drain(True)

    @pl.when(jnp.logical_not(is_src))
    def _():
        drain(False)
        for copy in swap1:
            copy.wait_send()

    for copy in swap2:
        copy.wait_send()


def solution(mesh):
    def step(adj, mask, h0, w1, w2):
        hbm = pl.BlockSpec(memory_space=pltpu.HBM)
        y_two = pl.pallas_call(
            kernel,
            name='gcn',
            out_shape=jax.ShapeDtypeStruct((BLOCK, F1), jnp.bfloat16),
            in_specs=[hbm] * 4,
            out_specs=pl.BlockSpec(memory_space=pltpu.VMEM),
            scratch_shapes=[
                pltpu.VMEM((BLOCK, 32 * BLOCK), jnp.bfloat16),
                pltpu.SMEM((64, 64), jnp.int32),
                pltpu.VMEM((F0, F1), jnp.bfloat16),
                pltpu.VMEM((F1, F0), jnp.bfloat16),
                pltpu.VMEM((SLOTS, F0, PART), jnp.bfloat16),
                pltpu.VMEM((SLOTS, F0, PART), jnp.bfloat16),
                pltpu.VMEM((BLOCK, 256), jnp.float32),
                pltpu.VMEM((BLOCK, F1), jnp.float32),
                pltpu.VMEM((BLOCK, 256), jnp.float32),
                pltpu.VMEM((BLOCK, F1), jnp.float32),
                pltpu.SemaphoreType.DMA((2,)),
                pltpu.SemaphoreType.DMA((BLOCK // BAND,)),
                pltpu.SemaphoreType.DMA((3,)),
                pltpu.SemaphoreType.DMA((SLOTS,)),
                pltpu.SemaphoreType.DMA((SLOTS,)),
                pltpu.SemaphoreType.DMA((2, 3)),
                pltpu.SemaphoreType.DMA((2, 3)),
                pltpu.SemaphoreType.DMA((2, 3)),
            ],
            compiler_params=pltpu.CompilerParams(
                collective_id=0, has_side_effects=True, vmem_limit_bytes=40 * 1024 * 1024),
        )(*[pltpu.with_memory_space_constraint(a, pltpu.HBM) for a in (adj, mask, h0.T, w1)])
        return jnp.dot(y_two, w2, preferred_element_type=jnp.float32)

    return jax.shard_map(step, mesh=mesh, in_specs=(P('rows', 'rep'), P(), P('rows', None), P(), P()),
                         out_specs=P('rows', None), check_vma=False)
```
